16 devices in a mesh: sys: 2 (over y, z), row: 8 (over x, core).
Axes of the slice: x: 4, y: 2, z: 1, core: 2. Of those that a mesh axis runs over, the one named last changes fastest.
The devices are a block of a 4x4x8 slice.
Arguments:
- positions: bfloat16 [32768, 256], P(('sys', 'row')), parts along dimension 0
- charges: float32 [32768], P(('sys', 'row')), parts along dimension 0
Outputs:
- output 1: float32 [32768, 256], P(('sys', 'row')), parts along dimension 0
- output 2: float32 [2], P('sys'), parts along dimension 0
There are 2 independent parts. The reference program is written for one: setup_inputs(seed, part) draws one part's arguments, and reference() takes and returns one part's arrays. A program takes and returns all parts, laid end to end along the dimension named above; each array names one.
All inputs are finite; a program needn't handle non-finite values.
Results may differ from the reference program's by a relative error of at most 0.001.
Values are sent between devices in bfloat16 or wider.
A program may use at most 768 MiB of HBM per device.

```python
import jax
import jax.numpy as jnp
from jax import lax

D = 256
ROWS_DEV = 2048
RING = 8
N_ROWS = ROWS_DEV * RING
ELL_SQ = float(D)


def setup_inputs(seed: int = 0, part: int = 0) -> dict:
    root_key = jax.random.key(seed)
    part_key = jax.random.fold_in(root_key, part)
    key_x, key_q = jax.random.split(part_key)
    positions = jax.random.normal(key_x, (N_ROWS, D), jnp.float32).astype(jnp.bfloat16)
    charges = jax.random.normal(key_q, (N_ROWS,), jnp.float32) * (N_ROWS ** -0.25)
    return {"positions": positions, "charges": charges}


def reference(positions, charges):
    sq_norm = jnp.sum(jnp.square(positions.astype(jnp.float32)), axis=1)
    blocks_x = positions.reshape(RING, ROWS_DEV, D)
    blocks_q = charges.reshape(RING, ROWS_DEV)
    blocks_sq = sq_norm.reshape(RING, ROWS_DEV)
    block_ids = jnp.arange(RING)
    local_ids = jnp.arange(ROWS_DEV)

    def row_block(host_in):
        host_x, host_q, host_sq, host_id = host_in

        def col_step(acc_state, col_in):
            force_acc, energy_acc = acc_state
            col_x, col_q, col_sq, col_id = col_in
            cross_dot = jnp.dot(host_x, col_x.T, preferred_element_type=jnp.float32)
            sq_dist = jnp.maximum(host_sq[:, None] + col_sq[None, :] - 2.0 * cross_dot, 0.0)
            is_self = (host_id * ROWS_DEV + local_ids)[:, None] == (col_id * ROWS_DEV + local_ids)[None, :]
            weight = jnp.where(is_self, 0.0, host_q[:, None] * col_q[None, :] * jnp.exp(-sq_dist / (2.0 * ELL_SQ)))
            pulled = jnp.dot(weight.astype(jnp.bfloat16), col_x, preferred_element_type=jnp.float32)
            force_acc = force_acc + jnp.sum(weight, axis=1)[:, None] * host_x.astype(jnp.float32) - pulled
            return (force_acc, energy_acc + jnp.sum(weight)), None

        init_state = (jnp.zeros((ROWS_DEV, D), jnp.float32), jnp.zeros((), jnp.float32))
        final_state, step_out = lax.scan(col_step, init_state, (blocks_x, blocks_q, blocks_sq, block_ids))
        return final_state

    forces, energies = lax.map(row_block, (blocks_x, blocks_q, blocks_sq, block_ids))
    return (forces / ELL_SQ).reshape(N_ROWS, D), (0.5 * jnp.sum(energies)).reshape(1)
```

```python
import functools
import math

import jax
import jax.numpy as jnp
from jax import lax
from jax.experimental import pallas as pl
from jax.experimental.pallas import tpu as pltpu
from jax.sharding import PartitionSpec as P

LANES = 128
QUANT = 256
SUBS = 4
HOST = 512


def kernel(cfg, x_hbm, q_ref, f_ref, e_ref, xs, aux, host_a, host_l, host_s, wts, acc, rsum, ebuf, load_sem, near_sem, relay_sem, sib_sem, aux_sem, e_sem, s_near, s_relay, s_fwd, s_sib, s_aux, s_e):
    groups, rows_dev, ring = cfg
    feat = x_hbm.shape[1]
    log2e = math.log2(math.e)
    dot_scale = 2.0 * log2e / (2.0 * feat)
    sq_scale = -log2e / (2.0 * feat)
    own_groups = rows_dev // (QUANT * SUBS)
    quanta = rows_dev // QUANT
    hosts = rows_dev // HOST
    chunks = rows_dev // LANES
    me = lax.axis_index("row")
    core = me % 2
    sib = me + 1 - 2 * core
    right = (me + 2) % ring
    left = (me + ring - 2) % ring
    right_x = (sib + 2) % ring
    left_x = (sib + ring - 2) % ring
    opp = (me + 4) % ring
    opp_x = (sib + 4) % ring

    def remote(src, dst, send, recv, dev):
        return pltpu.make_async_remote_copy(src_ref=src, dst_ref=dst, send_sem=send, recv_sem=recv, device_id={"row": dev}, device_id_type=pl.DeviceIdType.MESH)

    loads = [pltpu.make_async_copy(x_hbm.at[pl.ds(q * QUANT, QUANT), pl.ds(h * LANES, LANES)], xs.at[q // SUBS, q % SUBS, h], load_sem.at[q, h]) for q in range(quanta) for h in range(2)]
    for load in loads:
        load.start()
    barrier = pltpu.get_barrier_semaphore()
    for peer in (sib, right, left, right_x, left_x, opp, opp_x):
        pl.semaphore_signal(barrier, inc=1, device_id={"row": peer}, device_id_type=pl.DeviceIdType.MESH)
    for load in loads:
        load.wait()
    pl.semaphore_wait(barrier, 7)

    first = own_groups + 1

    def to_right(q):
        return remote(xs.at[q // SUBS, q % SUBS], xs.at[first + q, 0], s_near.at[q, 0], near_sem.at[first + q, 0], right)

    def to_left(q):
        return remote(xs.at[q // SUBS, q % SUBS], xs.at[first + q, 1], s_near.at[q, 1], near_sem.at[first + q, 1], left)

    sib_copies = [
        remote(xs.at[0], xs.at[own_groups], s_sib.at[0], sib_sem.at[0], sib),
        remote(xs.at[1, pl.ds(0, 2)], xs.at[first, pl.ds(2, 2)], s_sib.at[1], sib_sem.at[1], sib),
        remote(xs.at[1, pl.ds(2, 2)], xs.at[groups - 1, pl.ds(0, 2)], s_sib.at[2], sib_sem.at[2], sib),
    ]
    for copy in sib_copies:
        copy.start()
    for q in range(2):
        to_right(q).start()
        to_left(q).start()

    for c in range(chunks):
        g, s, r = c // (2 * SUBS), (c // 2) % SUBS, (c % 2) * LANES
        lo = xs[g, s, 0, pl.ds(r, LANES), :].astype(jnp.float32)
        hi = xs[g, s, 1, pl.ds(r, LANES), :].astype(jnp.float32)
        sq = jnp.sum(lo * lo + hi * hi, axis=1, keepdims=True)
        off = jnp.broadcast_to(sq * sq_scale, (LANES, LANES))
        q_row = q_ref[c : c + 1, :]
        aux[g, s, pl.ds(c % 2, 1), :] = jnp.transpose(off)[0:1, :]
        aux[g, s, pl.ds(2 + c % 2, 1), :] = q_row
        q_col = jnp.transpose(jnp.broadcast_to(q_row, (LANES, LANES)))
        mag = jnp.log(jnp.abs(q_col)) * log2e
        host_a[pl.ds(c * LANES, LANES), :] = off + mag
        host_l[pl.ds(c * LANES, LANES), :] = mag
        host_s[pl.ds(c * LANES, LANES), :] = jnp.where(q_col < 0.0, -1.0, 1.0)
    acc[...] = jnp.zeros_like(acc)
    rsum[...] = jnp.zeros_like(rsum)
    wts[1, ...] = jnp.zeros_like(wts[1, ...])

    far = first + quanta
    half = quanta // 2
    aux_plan = [
        (aux.at[0], aux.at[own_groups], sib),
        (aux.at[1, pl.ds(0, 2)], aux.at[first, pl.ds(2, 2)], sib),
        (aux.at[1, pl.ds(2, 2)], aux.at[groups - 1, pl.ds(0, 2)], sib),
    ]
    for h in range(2):
        aux_plan += [
            (aux.at[h], aux.at[pl.ds(first + half * h, half), 0], right),
            (aux.at[h], aux.at[pl.ds(first + half * h, half), 1], left),
            (aux.at[h], aux.at[pl.ds(first + 1 + half * h, half), 2], right_x),
            (aux.at[h], aux.at[pl.ds(first + 1 + half * h, half), 3], left_x),
            (aux.at[h], aux.at[pl.ds(far, half), h], opp),
            (aux.at[h], aux.at[pl.ds(far + 1, half), 2 + h], opp_x),
        ]
    aux_copies = [remote(src, dst, s_aux.at[n], aux_sem.at[n], dev) for n, (src, dst, dev) in enumerate(aux_plan)]
    for copy in aux_copies:
        copy.start()
    for q in range(2, quanta):
        to_right(q).start()
        to_left(q).start()

    def tile(g, s):
        return jnp.concatenate([xs[g, s, 0], xs[g, s, 1]], axis=1)

    def host_tile(t):
        return jnp.concatenate([tile(t * 2 // SUBS, t * 2 % SUBS), tile((t * 2 + 1) // SUBS, (t * 2 + 1) % SUBS)], axis=0)

    def weights(t, g, slot, diag):
        hx = host_tile(t)
        base = t * HOST
        for s in range(SUBS):
            dots = lax.dot_general(hx, tile(g, s), (((1,), (1,)), ((), ())), preferred_element_type=jnp.float32)
            step = LANES if diag else HOST
            for r in range(0, HOST, step):
                at = pl.ds(base + r, step)
                off, cap, total = host_a[at, :], host_l[at, :], rsum[at, :]
                for c in range(2):
                    power = dots[r : r + step, c * LANES : (c + 1) * LANES] * dot_scale + off + aux[g, s, pl.ds(c, 1), :]
                    w = jnp.exp2(jnp.minimum(power, cap)) * aux[g, s, pl.ds(2 + c, 1), :]
                    if diag and base + r == (g * SUBS + s) * QUANT + c * LANES:
                        same = lax.broadcasted_iota(jnp.int32, w.shape, 0) == lax.broadcasted_iota(jnp.int32, w.shape, 1)
                        w = jnp.where(same, 0.0, w)
                    total = total + w
                    wts[slot, 2 * s + c, pl.ds(r, step), :] = w.astype(jnp.bfloat16)
                rsum[at, :] = total

    def pull(t, g, slot):
        part = None
        for s in range(SUBS):
            w = jnp.concatenate([wts[slot, 2 * s], wts[slot, 2 * s + 1]], axis=1)
            d = jnp.dot(w, tile(g, s), preferred_element_type=jnp.float32)
            part = d if part is None else part + d
        acc[pl.ds(t * HOST, HOST), :] += part

    def group(g, before, diag=False):
        for t in range(hosts):
            if t == 0:
                pull(hosts - 1, before, 1)
            else:
                pull(t - 1, g, (t - 1) % 2)
            weights(t, g, t % 2, diag)

    group(0, 0, True)
    group(1, 0, True)

    def near_in(g, d):
        return remote(xs.at[g, d], xs.at[g, d], s_near.at[0, d], near_sem.at[g, d], me)

    def relay(g):
        return remote(xs.at[g, pl.ds(0, 2)], xs.at[g + 1, pl.ds(2, 2)], s_relay.at[g], relay_sem.at[g + 1], sib)

    def forward_right(g):
        return remote(xs.at[g, 0], xs.at[g + quanta, 0], s_fwd.at[g], near_sem.at[g + quanta, 0], right)

    def forward_left(g):
        return remote(xs.at[g, 1], xs.at[g + half, 1], s_fwd.at[g], near_sem.at[g + half, 1], left)

    last = groups - 1
    for copy in sib_copies:
        copy.wait_recv()
    for copy in aux_copies:
        copy.wait_recv()

    def step(g, carry):
        @pl.when((g >= first) & (g < last))
        def _():
            near_in(g, 0).wait_recv()
            near_in(g, 1).wait_recv()
            relay(g).start()

        @pl.when((g >= first) & (g < first + half))
        def _():
            forward_right(g).start()

        @pl.when((g >= first + half) & (g < first + quanta))
        def _():
            forward_left(g).start()

        @pl.when(g > first)
        def _():
            remote(xs.at[g, pl.ds(2, 2)], xs.at[g, pl.ds(2, 2)], s_relay.at[0], relay_sem.at[g], me).wait_recv()

        group(g, g - 1)
        return carry

    lax.fori_loop(own_groups, groups, step, 0)
    energy = jnp.zeros((8, LANES), jnp.float32)
    for r in range(0, rows_dev, HOST):
        at = pl.ds(r, HOST)
        energy = energy + jnp.sum((rsum[at, :] * host_s[at, :]).reshape(HOST // 8, 8, LANES), axis=0)
    ebuf[me] = energy
    pull(hosts - 1, last, 1)
    e_copies = [remote(ebuf.at[me], ebuf.at[me], s_e.at[d], e_sem.at[d], (me + d) % ring) for d in range(1, ring)]
    for copy in e_copies:
        copy.start()
    for t in range(hosts):
        at = pl.ds(t * HOST, HOST)
        total = jnp.sum(rsum[at, :], axis=1, keepdims=True)
        sign = host_s[at, :] * (1.0 / feat)
        hx = host_tile(t).astype(jnp.float32)
        f_ref[at, :] = (total * hx - acc[at, :]) * jnp.concatenate([sign, sign], axis=1)

    for q in range(quanta):
        to_right(q).wait_send()
        to_left(q).wait_send()
    for copy in sib_copies + aux_copies:
        copy.wait_send()

    def drain(g, carry):
        relay(g).wait_send()
        return carry

    lax.fori_loop(first, last, drain, 0)

    def drain_right(g, carry):
        forward_right(g).wait_send()
        return carry

    lax.fori_loop(first, first + half, drain_right, 0)

    def drain_left(g, carry):
        forward_left(g).wait_send()
        return carry

    lax.fori_loop(first + half, first + quanta, drain_left, 0)
    for copy in e_copies:
        copy.wait()
    whole = ebuf[0]
    for d in range(1, ring):
        whole = whole + ebuf[d]
    e_ref[0] = 0.5 * jnp.sum(whole)


def solution(mesh):
    ring = mesh.shape["row"]

    def device_body(pos, chg):
        rows, feat = pos.shape
        groups = ring * rows // (QUANT * SUBS)
        quanta = rows // QUANT
        assert ring == 8 and feat == 2 * LANES and quanta == 8
        dma = pltpu.SemaphoreType.DMA
        f32 = jnp.float32
        vmem = pltpu.VMEM
        scratch = [
            vmem((groups, SUBS, 2, QUANT, LANES), jnp.bfloat16),
            vmem((groups, SUBS, 4, LANES), f32),
            vmem((rows, LANES), f32),
            vmem((rows, LANES), f32),
            vmem((rows, LANES), f32),
            vmem((2, 2 * SUBS, HOST, LANES), jnp.bfloat16),
            vmem((rows, feat), f32),
            vmem((rows, LANES), f32),
            vmem((ring, 8, LANES), f32),
            dma((quanta, 2)),
            dma((groups, 2)),
            dma((groups,)),
            dma((3,)),
            dma((15,)),
            dma((ring,)),
            dma((quanta, 2)),
            dma((groups,)),
            dma((groups,)),
            dma((3,)),
            dma((15,)),
            dma((ring,)),
        ]
        forces, energy = pl.pallas_call(
            functools.partial(kernel, (groups, rows, ring)),
            out_shape=(jax.ShapeDtypeStruct((rows, feat), f32), jax.ShapeDtypeStruct((1,), f32)),
            in_specs=[pl.BlockSpec(memory_space=pltpu.HBM), pl.BlockSpec(memory_space=pltpu.VMEM)],
            out_specs=(pl.BlockSpec(memory_space=pltpu.VMEM), pl.BlockSpec(memory_space=pltpu.SMEM)),
            scratch_shapes=scratch,
            compiler_params=pltpu.CompilerParams(collective_id=0, has_side_effects=True, vmem_limit_bytes=63 * 2**20 - 2**19),
            name="pair_forces",
        )(pos, chg.reshape(rows // LANES, LANES))
        return forces, energy

    return jax.shard_map(device_body, mesh=mesh, in_specs=(P(("sys", "row"), None), P(("sys", "row"))), out_specs=(P(("sys", "row"), None), P("sys")), check_vma=False)
```

```python
import functools
import math

import jax
import jax.numpy as jnp
from jax import lax
from jax.experimental import pallas as pl
from jax.experimental.pallas import tpu as pltpu
from jax.sharding import PartitionSpec as P

LANES = 128
QUANT = 256
SUBS = 4
HOST = 512
NEAR = [(0, 2), (2, 2), (4, 2), (6, 2)]
FAR = [(8, 2), (10, 1), (11, 1)]


def kernel(cfg, x_ref, q_ref, f_ref, e_ref, xs, aux, host_a, host_l, host_s, wts, acc, rsum, ebuf, near_sem, far_sem, relay_sem, sib_sem, aux_sem, e_sem, s_near, s_far, s_relay, s_sib, s_aux, s_e):
    groups, rows_dev, ring = cfg
    feat = x_ref.shape[2]
    log2e = math.log2(math.e)
    dot_scale = 2.0 * log2e / (2.0 * feat)
    sq_scale = -log2e / (2.0 * feat)
    own_groups = rows_dev // (QUANT * SUBS)
    quanta = rows_dev // QUANT
    hosts = rows_dev // HOST
    chunks = rows_dev // LANES
    me = lax.axis_index("row")
    core = me % 2
    sib = me + 1 - 2 * core
    right = (me + 2) % ring
    left = (me + ring - 2) % ring
    right_x = (sib + 2) % ring
    left_x = (sib + ring - 2) % ring
    opp = (me + 4) % ring
    opp_x = (sib + 4) % ring

    def remote(src, dst, send, recv, dev):
        return pltpu.make_async_remote_copy(src_ref=src, dst_ref=dst, send_sem=send, recv_sem=recv, device_id={"row": dev}, device_id_type=pl.DeviceIdType.MESH)

    barrier = pltpu.get_barrier_semaphore()
    for peer in (sib, right, left, right_x, left_x, opp, opp_x):
        pl.semaphore_signal(barrier, inc=1, device_id={"row": peer}, device_id_type=pl.DeviceIdType.MESH)

    first = own_groups + 1
    half = quanta // 2
    far = first + quanta
    last = groups - 1

    def both_halves(q, n, group, sub, send, recv, dev):
        return [remote(x_ref.at[pl.ds(q, n), :, pl.ds(h * LANES, LANES)], xs.at[pl.ds(group, n), sub, h], send.at[h], recv.at[h], dev) for h in range(2)]

    def within(q, n, group, sub, send, recv, dev):
        return [remote(x_ref.at[pl.ds(q, n), :, pl.ds(h * LANES, LANES)], xs.at[group, pl.ds(sub, n), h], send.at[h], recv.at[h], dev) for h in range(2)]

    near = {}
    for n, (m, size) in enumerate(NEAR):
        near[first + m] = both_halves(m, size, first + m, 0, s_near.at[n, 0], near_sem.at[n, 0], right) + both_halves((m + half) % quanta, size, first + m, 1, s_near.at[n, 1], near_sem.at[n, 1], left)
    sib_copies = within(0, 4, own_groups, 0, s_sib.at[0], sib_sem.at[0], sib) + within(4, 2, first, 2, s_sib.at[1], sib_sem.at[1], sib) + within(6, 2, last, 0, s_sib.at[2], sib_sem.at[2], sib)
    forward = {}
    for n, (m, size) in enumerate(FAR):
        src, dst = first + m - quanta, first + m
        forward[dst] = [remote(xs.at[pl.ds(src, size), d], xs.at[pl.ds(dst, size), d], s_far.at[n, d], far_sem.at[n, d], (right, left)[d]) for d in range(2)]
    relays = {first + m: remote(xs.at[pl.ds(first + m, size), pl.ds(0, 2)], xs.at[pl.ds(first + m + 1, size), pl.ds(2, 2)], s_relay.at[n], relay_sem.at[n], sib) for n, (m, size) in enumerate(NEAR + FAR)}

    pl.semaphore_wait(barrier, 7)
    starts = list(near)
    for copy in near[starts[0]] + sib_copies + near[starts[1]]:
        copy.start()

    for g in range(own_groups):
        for s in range(SUBS):
            for h in range(2):
                xs[g, s, h] = x_ref[g * SUBS + s, :, h * LANES : (h + 1) * LANES]

    eye = lax.broadcasted_iota(jnp.int32, (LANES, LANES), 0) == lax.broadcasted_iota(jnp.int32, (LANES, LANES), 1)
    for c in range(chunks):
        g, s, r = c // (2 * SUBS), (c // 2) % SUBS, (c % 2) * LANES
        lo = xs[g, s, 0, pl.ds(r, LANES), :].astype(jnp.float32)
        hi = xs[g, s, 1, pl.ds(r, LANES), :].astype(jnp.float32)
        off = jnp.sum(lo * lo + hi * hi, axis=1, keepdims=True) * sq_scale
        q_row = q_ref[c : c + 1, :]
        aux[g, s, pl.ds(c % 2, 1), :] = jnp.sum(jnp.where(eye, off, 0.0), axis=0, keepdims=True)
        aux[g, s, pl.ds(2 + c % 2, 1), :] = q_row
        q_col = jnp.sum(jnp.where(eye, q_row, 0.0), axis=1, keepdims=True)
        mag = jnp.log(jnp.abs(q_col)) * log2e
        wide = (LANES, LANES)
        host_a[pl.ds(c * LANES, LANES), :] = jnp.broadcast_to(off + mag, wide)
        host_l[pl.ds(c * LANES, LANES), :] = jnp.broadcast_to(mag, wide)
        host_s[pl.ds(c * LANES, LANES), :] = jnp.broadcast_to(jnp.where(q_col < 0.0, -1.0, 1.0), wide)
    acc[...] = jnp.zeros_like(acc)
    rsum[...] = jnp.zeros_like(rsum)
    wts[1, ...] = jnp.zeros_like(wts[1, ...])

    aux_plan = [
        (aux.at[0], aux.at[own_groups], sib),
        (aux.at[1, pl.ds(0, 2)], aux.at[first, pl.ds(2, 2)], sib),
        (aux.at[1, pl.ds(2, 2)], aux.at[last, pl.ds(0, 2)], sib),
    ]
    for h in range(2):
        at, turned = first + half * h, first + half * (1 - h)
        aux_plan += [
            (aux.at[h], aux.at[pl.ds(at, half), 0], right),
            (aux.at[h], aux.at[pl.ds(turned, half), 1], left),
            (aux.at[h], aux.at[pl.ds(at + 1, half), 2], right_x),
            (aux.at[h], aux.at[pl.ds(turned + 1, half), 3], left_x),
            (aux.at[h], aux.at[pl.ds(far, half), h], opp),
            (aux.at[h], aux.at[pl.ds(far + 1, half), 2 + h], opp_x),
        ]
    aux_copies = [remote(src, dst, s_aux.at[n], aux_sem.at[n], dev) for n, (src, dst, dev) in enumerate(aux_plan)]
    for copy in aux_copies:
        copy.start()
    for g in starts[2:]:
        for copy in near[g]:
            copy.start()

    def tile(g, s):
        return jnp.concatenate([xs[g, s, 0], xs[g, s, 1]], axis=1)

    def host_tile(t):
        return jnp.concatenate([tile(t * 2 // SUBS, t * 2 % SUBS), tile((t * 2 + 1) // SUBS, (t * 2 + 1) % SUBS)], axis=0)

    def weights(t, subs, slot, diag):
        hx = host_tile(t)
        base = t * HOST
        for n, (g, s) in enumerate(subs):
            dots = lax.dot_general(hx, tile(g, s), (((1,), (1,)), ((), ())), preferred_element_type=jnp.float32)
            step = LANES if diag else HOST
            for r in range(0, HOST, step):
                at = pl.ds(base + r, step)
                off, cap, total = host_a[at, :], host_l[at, :], rsum[at, :]
                for c in range(2):
                    power = dots[r : r + step, c * LANES : (c + 1) * LANES] * dot_scale + off + aux[g, s, pl.ds(c, 1), :]
                    w = jnp.exp2(jnp.minimum(power, cap)) * aux[g, s, pl.ds(2 + c, 1), :]
                    if diag and base + r == (g * SUBS + s) * QUANT + c * LANES:
                        w = jnp.where(eye, 0.0, w)
                    total = total + w
                    wts[slot, 2 * n + c, pl.ds(r, step), :] = w.astype(jnp.bfloat16)
                rsum[at, :] = total

    def pull(t, subs, slot):
        part = None
        for n, (g, s) in enumerate(subs):
            w = jnp.concatenate([wts[slot, 2 * n], wts[slot, 2 * n + 1]], axis=1)
            d = jnp.dot(w, tile(g, s), preferred_element_type=jnp.float32)
            part = d if part is None else part + d
        acc[pl.ds(t * HOST, HOST), :] += part

    def visit(subs, before, diag=False):
        for t in range(hosts):
            if t == 0:
                pull(hosts - 1, before, 1)
            else:
                pull(t - 1, subs, (t - 1) % 2)
            weights(t, subs, t % 2, diag)

    def all_of(g):
        return [(g, s) for s in range(SUBS)]

    visit(all_of(0), all_of(0), True)
    visit(all_of(1), all_of(0), True)
    for copy in sib_copies + aux_copies:
        copy.wait_recv()

    def step(g, carry):
        for at in (*near, *forward):
            if at == last - 1:
                continue

            @pl.when(g == at)
            def _():
                for copy in near.get(at) or forward[at]:
                    copy.wait_recv()
                relays[at].start()
                for dst in forward:
                    src = dst - quanta
                    if at in near and max(a for a in near if a <= src) == at:
                        for copy in forward[dst]:
                            copy.start()

        for at, copy in relays.items():

            @pl.when(g == at + 1)
            def _():
                copy.wait_recv()

        visit(all_of(g), all_of(g - 1))
        return carry

    lax.fori_loop(own_groups, last - 1, step, 0)
    relays[last - 2].wait_recv()
    rest = [(last, 0), (last, 1), (last - 1, 2), (last - 1, 3)]
    visit(rest, all_of(last - 2))
    for copy in forward[last - 1]:
        copy.wait_recv()
    relays[last - 1].start()
    late = [(last - 1, 0), (last - 1, 1)]
    visit(late, rest)
    relays[last - 1].wait_recv()
    end = [(last, 2), (last, 3)]
    visit(end, late)
    energy = jnp.zeros((8, LANES), jnp.float32)
    for r in range(0, rows_dev, HOST):
        at = pl.ds(r, HOST)
        energy = energy + jnp.sum((rsum[at, :] * host_s[at, :]).reshape(HOST // 8, 8, LANES), axis=0)
    ebuf[me] = energy
    pull(hosts - 1, end, 1)
    e_copies = [remote(ebuf.at[me], ebuf.at[me], s_e.at[d], e_sem.at[d], (me + d) % ring) for d in range(1, ring)]
    for copy in e_copies:
        copy.start()
    for t in range(hosts):
        at = pl.ds(t * HOST, HOST)
        total = jnp.sum(rsum[at, :], axis=1, keepdims=True)
        sign = host_s[at, :] * (1.0 / feat)
        hx = host_tile(t).astype(jnp.float32)
        f_ref[at, :] = (total * hx - acc[at, :]) * jnp.concatenate([sign, sign], axis=1)

    for copies in (*near.values(), *forward.values(), sib_copies, aux_copies, relays.values()):
        for copy in copies:
            copy.wait_send()
    for copy in e_copies:
        copy.wait()
    whole = ebuf[0]
    for d in range(1, ring):
        whole = whole + ebuf[d]
    e_ref[0] = 0.5 * jnp.sum(whole)


def solution(mesh):
    ring = mesh.shape["row"]

    def device_body(pos, chg):
        rows, feat = pos.shape
        groups = ring * rows // (QUANT * SUBS)
        quanta = rows // QUANT
        assert ring == 8 and feat == 2 * LANES and quanta == 8
        dma = pltpu.SemaphoreType.DMA
        f32 = jnp.float32
        vmem = pltpu.VMEM
        scratch = [
            vmem((groups, SUBS, 2, QUANT, LANES), jnp.bfloat16),
            vmem((groups, SUBS, 4, LANES), f32),
            vmem((rows, LANES), f32),
            vmem((rows, LANES), f32),
            vmem((rows, LANES), f32),
            vmem((2, 2 * SUBS, HOST, LANES), jnp.bfloat16),
            vmem((rows, feat), f32),
            vmem((rows, LANES), f32),
            vmem((ring, 8, LANES), f32),
        ]
        for _ in range(2):
            scratch += [dma((len(NEAR), 2, 2)), dma((len(FAR), 2)), dma((len(NEAR + FAR),)), dma((3, 2)), dma((15,)), dma((ring,))]
        forces, energy = pl.pallas_call(
            functools.partial(kernel, (groups, rows, ring)),
            out_shape=(jax.ShapeDtypeStruct((rows, feat), f32), jax.ShapeDtypeStruct((1,), f32)),
            in_specs=[pl.BlockSpec(memory_space=pltpu.VMEM), pl.BlockSpec(memory_space=pltpu.VMEM)],
            out_specs=(pl.BlockSpec(memory_space=pltpu.VMEM), pl.BlockSpec(memory_space=pltpu.SMEM)),
            scratch_shapes=scratch,
            compiler_params=pltpu.CompilerParams(collective_id=0, has_side_effects=True, vmem_limit_bytes=40 * 2**20),
            name="pair_forces",
        )(pos.reshape(quanta, QUANT, feat), chg.reshape(rows // LANES, LANES))
        return forces, energy

    return jax.shard_map(device_body, mesh=mesh, in_specs=(P(("sys", "row"), None), P(("sys", "row"))), out_specs=(P(("sys", "row"), None), P("sys")), check_vma=False)
```

```python
import functools
import math

import jax
import jax.numpy as jnp
from jax import lax
from jax.experimental import pallas as pl
from jax.experimental.pallas import tpu as pltpu
from jax.sharding import PartitionSpec as P

LANES = 128
QUANT = 256
SUBS = 4
HOST = 512
NEAR = [(0, 2), (2, 2), (4, 2), (6, 2)]
FAR = [(8, 2), (10, 1), (11, 1)]


def kernel(cfg, x_ref, q_ref, f_ref, e_ref, xs, aux, host_a, host_l, host_s, wts, acc, rsum, ebuf, load_sem, near_sem, far_sem, relay_sem, sib_sem, aux_sem, e_sem, s_near, s_far, s_relay, s_sib, s_aux, s_e):
    groups, rows_dev, ring = cfg
    feat = x_ref.shape[1]
    log2e = math.log2(math.e)
    dot_scale = 2.0 * log2e / (2.0 * feat)
    sq_scale = -log2e / (2.0 * feat)
    own_groups = rows_dev // (QUANT * SUBS)
    quanta = rows_dev // QUANT
    hosts = rows_dev // HOST
    chunks = rows_dev // LANES
    me = lax.axis_index("row")
    core = me % 2
    sib = me + 1 - 2 * core
    right = (me + 2) % ring
    left = (me + ring - 2) % ring
    right_x = (sib + 2) % ring
    left_x = (sib + ring - 2) % ring
    opp = (me + 4) % ring
    opp_x = (sib + 4) % ring

    def remote(src, dst, send, recv, dev):
        return pltpu.make_async_remote_copy(src_ref=src, dst_ref=dst, send_sem=send, recv_sem=recv, device_id={"row": dev}, device_id_type=pl.DeviceIdType.MESH)

    barrier = pltpu.get_barrier_semaphore()
    for peer in (sib, right, left, right_x, left_x, opp, opp_x):
        pl.semaphore_signal(barrier, inc=1, device_id={"row": peer}, device_id_type=pl.DeviceIdType.MESH)

    first = own_groups + 1
    half = quanta // 2
    far = first + quanta
    last = groups - 1

    loads = [pltpu.make_async_copy(x_ref.at[pl.ds(q * QUANT, QUANT), pl.ds(h * LANES, LANES)], xs.at[q // SUBS, q % SUBS, h], load_sem.at[q, h]) for q in (0, 1, 4, 5, 2, 3, 6, 7) for h in range(2)]
    for load in loads:
        load.start()

    def own(q, n):
        return xs.at[q // SUBS, pl.ds(q % SUBS, n)]

    near = {}
    for n, (m, size) in enumerate(NEAR):
        near[first + m] = [remote(own((m + d * half) % quanta, size), xs.at[pl.ds(first + m, size), d], s_near.at[n, d], near_sem.at[n, d], (right, left)[d]) for d in range(2)]
    sib_copies = [remote(own(q, n), dst, s_sib.at[k], sib_sem.at[k], sib) for k, (q, n, dst) in enumerate([(0, 4, xs.at[own_groups]), (4, 2, xs.at[first, pl.ds(2, 2)]), (6, 2, xs.at[last, pl.ds(0, 2)])])]
    forward = {}
    for n, (m, size) in enumerate(FAR):
        src, dst = first + m - quanta, first + m
        forward[dst] = [remote(xs.at[pl.ds(src, size), d], xs.at[pl.ds(dst, size), d], s_far.at[n, d], far_sem.at[n, d], (right, left)[d]) for d in range(2)]
    relays = {first + m: remote(xs.at[pl.ds(first + m, size), pl.ds(0, 2)], xs.at[pl.ds(first + m + 1, size), pl.ds(2, 2)], s_relay.at[n], relay_sem.at[n], sib) for n, (m, size) in enumerate(NEAR + FAR)}

    starts = list(near)
    for load in loads[:8]:
        load.wait()
    pl.semaphore_wait(barrier, 7)
    for copy in near[starts[0]]:
        copy.start()
    for load in loads[8:]:
        load.wait()
    for copy in sib_copies + near[starts[1]]:
        copy.start()

    eye = lax.broadcasted_iota(jnp.int32, (LANES, LANES), 0) == lax.broadcasted_iota(jnp.int32, (LANES, LANES), 1)
    for c in range(chunks):
        g, s, r = c // (2 * SUBS), (c // 2) % SUBS, (c % 2) * LANES
        lo = xs[g, s, 0, pl.ds(r, LANES), :].astype(jnp.float32)
        hi = xs[g, s, 1, pl.ds(r, LANES), :].astype(jnp.float32)
        off = jnp.sum(lo * lo + hi * hi, axis=1, keepdims=True) * sq_scale
        q_row = q_ref[c : c + 1, :]
        aux[g, s, pl.ds(c % 2, 1), :] = jnp.sum(jnp.where(eye, off, 0.0), axis=0, keepdims=True)
        aux[g, s, pl.ds(2 + c % 2, 1), :] = q_row
        q_col = jnp.sum(jnp.where(eye, q_row, 0.0), axis=1, keepdims=True)
        mag = jnp.log(jnp.abs(q_col)) * log2e
        wide = (LANES, LANES)
        host_a[pl.ds(c * LANES, LANES), :] = jnp.broadcast_to(off + mag, wide)
        host_l[pl.ds(c * LANES, LANES), :] = jnp.broadcast_to(mag, wide)
        host_s[pl.ds(c * LANES, LANES), :] = jnp.broadcast_to(jnp.where(q_col < 0.0, -1.0, 1.0), wide)
    acc[...] = jnp.zeros_like(acc)
    rsum[...] = jnp.zeros_like(rsum)
    wts[1, ...] = jnp.zeros_like(wts[1, ...])

    aux_plan = [
        (aux.at[0], aux.at[own_groups], sib),
        (aux.at[1, pl.ds(0, 2)], aux.at[first, pl.ds(2, 2)], sib),
        (aux.at[1, pl.ds(2, 2)], aux.at[last, pl.ds(0, 2)], sib),
    ]
    for h in range(2):
        at, turned = first + half * h, first + half * (1 - h)
        aux_plan += [
            (aux.at[h], aux.at[pl.ds(at, half), 0], right),
            (aux.at[h], aux.at[pl.ds(turned, half), 1], left),
            (aux.at[h], aux.at[pl.ds(at + 1, half), 2], right_x),
            (aux.at[h], aux.at[pl.ds(turned + 1, half), 3], left_x),
            (aux.at[h], aux.at[pl.ds(far, half), h], opp),
            (aux.at[h], aux.at[pl.ds(far + 1, half), 2 + h], opp_x),
        ]
    aux_copies = [remote(src, dst, s_aux.at[n], aux_sem.at[n], dev) for n, (src, dst, dev) in enumerate(aux_plan)]
    for copy in aux_copies:
        copy.start()
    for g in starts[2:]:
        for copy in near[g]:
            copy.start()

    def tile(g, s):
        return jnp.concatenate([xs[g, s, 0], xs[g, s, 1]], axis=1)

    def host_tile(t):
        return jnp.concatenate([tile(t * 2 // SUBS, t * 2 % SUBS), tile((t * 2 + 1) // SUBS, (t * 2 + 1) % SUBS)], axis=0)

    def weights(t, subs, slot, diag):
        hx = host_tile(t)
        base = t * HOST
        for n, (g, s) in enumerate(subs):
            dots = lax.dot_general(hx, tile(g, s), (((1,), (1,)), ((), ())), preferred_element_type=jnp.float32)
            step = LANES if diag else HOST
            for r in range(0, HOST, step):
                at = pl.ds(base + r, step)
                off, cap, total = host_a[at, :], host_l[at, :], rsum[at, :]
                for c in range(2):
                    power = dots[r : r + step, c * LANES : (c + 1) * LANES] * dot_scale + off + aux[g, s, pl.ds(c, 1), :]
                    w = jnp.exp2(jnp.minimum(power, cap)) * aux[g, s, pl.ds(2 + c, 1), :]
                    if diag and base + r == (g * SUBS + s) * QUANT + c * LANES:
                        w = jnp.where(eye, 0.0, w)
                    total = total + w
                    wts[slot, 2 * n + c, pl.ds(r, step), :] = w.astype(jnp.bfloat16)
                rsum[at, :] = total

    def pull(t, subs, slot):
        part = None
        for n, (g, s) in enumerate(subs):
            w = jnp.concatenate([wts[slot, 2 * n], wts[slot, 2 * n + 1]], axis=1)
            d = jnp.dot(w, tile(g, s), preferred_element_type=jnp.float32)
            part = d if part is None else part + d
        acc[pl.ds(t * HOST, HOST), :] += part

    def visit(subs, before, diag=False):
        for t in range(hosts):
            if t == 0:
                pull(hosts - 1, before, 1)
            else:
                pull(t - 1, subs, (t - 1) % 2)
            weights(t, subs, t % 2, diag)

    def all_of(g):
        return [(g, s) for s in range(SUBS)]

    visit(all_of(0), all_of(0), True)
    visit(all_of(1), all_of(0), True)
    for copy in sib_copies + aux_copies:
        copy.wait_recv()

    def step(g, carry):
        for at in (*near, *forward):
            if at == last - 1:
                continue

            @pl.when(g == at)
            def _():
                for copy in near.get(at) or forward[at]:
                    copy.wait_recv()
                relays[at].start()
                for dst in forward:
                    src = dst - quanta
                    if at in near and max(a for a in near if a <= src) == at:
                        for copy in forward[dst]:
                            copy.start()

        for at, copy in relays.items():

            @pl.when(g == at + 1)
            def _():
                copy.wait_recv()

        visit(all_of(g), all_of(g - 1))
        return carry

    lax.fori_loop(own_groups, last - 1, step, 0)
    relays[last - 2].wait_recv()
    rest = [(last, 0), (last, 1), (last - 1, 2), (last - 1, 3)]
    visit(rest, all_of(last - 2))
    for copy in forward[last - 1]:
        copy.wait_recv()
    relays[last - 1].start()
    late = [(last - 1, 0), (last - 1, 1)]
    visit(late, rest)
    relays[last - 1].wait_recv()
    end = [(last, 2), (last, 3)]
    visit(end, late)
    energy = jnp.zeros((8, LANES), jnp.float32)
    for r in range(0, rows_dev, HOST):
        at = pl.ds(r, HOST)
        energy = energy + jnp.sum((rsum[at, :] * host_s[at, :]).reshape(HOST // 8, 8, LANES), axis=0)
    ebuf[me] = energy
    pull(hosts - 1, end, 1)
    e_copies = [remote(ebuf.at[me], ebuf.at[me], s_e.at[d], e_sem.at[d], (me + d) % ring) for d in range(1, ring)]
    for copy in e_copies:
        copy.start()
    for t in range(hosts):
        at = pl.ds(t * HOST, HOST)
        total = jnp.sum(rsum[at, :], axis=1, keepdims=True)
        sign = host_s[at, :] * (1.0 / feat)
        hx = host_tile(t).astype(jnp.float32)
        f_ref[at, :] = (total * hx - acc[at, :]) * jnp.concatenate([sign, sign], axis=1)

    for copies in (*near.values(), *forward.values(), sib_copies, aux_copies, relays.values()):
        for copy in copies:
            copy.wait_send()
    for copy in e_copies:
        copy.wait()
    whole = ebuf[0]
    for d in range(1, ring):
        whole = whole + ebuf[d]
    e_ref[0] = 0.5 * jnp.sum(whole)


def solution(mesh):
    ring = mesh.shape["row"]

    def device_body(pos, chg):
        rows, feat = pos.shape
        groups = ring * rows // (QUANT * SUBS)
        quanta = rows // QUANT
        assert ring == 8 and feat == 2 * LANES and quanta == 8
        dma = pltpu.SemaphoreType.DMA
        f32 = jnp.float32
        vmem = pltpu.VMEM
        scratch = [
            vmem((groups, SUBS, 2, QUANT, LANES), jnp.bfloat16),
            vmem((groups, SUBS, 4, LANES), f32),
            vmem((rows, LANES), f32),
            vmem((rows, LANES), f32),
            vmem((rows, LANES), f32),
            vmem((2, 2 * SUBS, HOST, LANES), jnp.bfloat16),
            vmem((rows, feat), f32),
            vmem((rows, LANES), f32),
            vmem((ring, 8, LANES), f32),
            dma((quanta, 2)),
        ]
        for _ in range(2):
            scratch += [dma((len(NEAR), 2)), dma((len(FAR), 2)), dma((len(NEAR + FAR),)), dma((3,)), dma((15,)), dma((ring,))]
        forces, energy = pl.pallas_call(
            functools.partial(kernel, (groups, rows, ring)),
            out_shape=(jax.ShapeDtypeStruct((rows, feat), f32), jax.ShapeDtypeStruct((1,), f32)),
            in_specs=[pl.BlockSpec(memory_space=pltpu.HBM), pl.BlockSpec(memory_space=pltpu.VMEM)],
            out_specs=(pl.BlockSpec(memory_space=pltpu.VMEM), pl.BlockSpec(memory_space=pltpu.SMEM)),
            scratch_shapes=scratch,
            compiler_params=pltpu.CompilerParams(collective_id=0, has_side_effects=True, vmem_limit_bytes=63 * 2**20 - 2**19),
            name="pair_forces",
        )(pos, chg.reshape(rows // LANES, LANES))
        return forces, energy

    return jax.shard_map(device_body, mesh=mesh, in_specs=(P(("sys", "row"), None), P(("sys", "row"))), out_specs=(P(("sys", "row"), None), P("sys")), check_vma=False)
```

```python
import functools
import math

import jax
import jax.numpy as jnp
from jax import lax
from jax.experimental import pallas as pl
from jax.experimental.pallas import tpu as pltpu
from jax.sharding import PartitionSpec as P

LANES = 128
QUANT = 256
SUBS = 4
HOST = 512
NEAR = [(m, 1) for m in range(8)]
FAR = [(m, 1) for m in range(8, 12)]


def kernel(cfg, x_ref, q_ref, f_ref, e_ref, xs, aux, host_a, host_l, host_s, wts, acc, rsum, ebuf, load_sem, near_sem, far_sem, relay_sem, sib_sem, aux_sem, e_sem, s_near, s_far, s_relay, s_sib, s_aux, s_e):
    groups, rows_dev, ring = cfg
    feat = x_ref.shape[1]
    log2e = math.log2(math.e)
    dot_scale = 2.0 * log2e / (2.0 * feat)
    sq_scale = -log2e / (2.0 * feat)
    own_groups = rows_dev // (QUANT * SUBS)
    quanta = rows_dev // QUANT
    hosts = rows_dev // HOST
    chunks = rows_dev // LANES
    me = lax.axis_index("row")
    core = me % 2
    sib = me + 1 - 2 * core
    right = (me + 2) % ring
    left = (me + ring - 2) % ring
    right_x = (sib + 2) % ring
    left_x = (sib + ring - 2) % ring
    opp = (me + 4) % ring
    opp_x = (sib + 4) % ring

    def remote(src, dst, send, recv, dev):
        return pltpu.make_async_remote_copy(src_ref=src, dst_ref=dst, send_sem=send, recv_sem=recv, device_id={"row": dev}, device_id_type=pl.DeviceIdType.MESH)

    barrier = pltpu.get_barrier_semaphore()
    for peer in (sib, right, left, right_x, left_x, opp, opp_x):
        pl.semaphore_signal(barrier, inc=1, device_id={"row": peer}, device_id_type=pl.DeviceIdType.MESH)

    first = own_groups + 1
    half = quanta // 2
    far = first + quanta
    last = groups - 1

    loads = [pltpu.make_async_copy(x_ref.at[pl.ds(q * QUANT, QUANT), pl.ds(h * LANES, LANES)], xs.at[q // SUBS, q % SUBS, h], load_sem.at[q, h]) for q in (0, 1, 4, 5, 2, 3, 6, 7) for h in range(2)]
    for load in loads:
        load.start()

    def own(q, n):
        return xs.at[q // SUBS, pl.ds(q % SUBS, n)]

    near = {}
    for n, (m, size) in enumerate(NEAR):
        near[first + m] = [remote(own((m + d * half) % quanta, size), xs.at[pl.ds(first + m, size), d], s_near.at[n, d], near_sem.at[n, d], (right, left)[d]) for d in range(2)]
    sib_copies = [remote(own(q, n), dst, s_sib.at[k], sib_sem.at[k], sib) for k, (q, n, dst) in enumerate([(0, 4, xs.at[own_groups]), (4, 2, xs.at[first, pl.ds(2, 2)]), (6, 2, xs.at[last, pl.ds(0, 2)])])]
    forward = {}
    for n, (m, size) in enumerate(FAR):
        src, dst = first + m - quanta, first + m
        forward[dst] = [remote(xs.at[pl.ds(src, size), d], xs.at[pl.ds(dst, size), d], s_far.at[n, d], far_sem.at[n, d], (right, left)[d]) for d in range(2)]
    relays = {first + m: remote(xs.at[pl.ds(first + m, size), pl.ds(0, 2)], xs.at[pl.ds(first + m + 1, size), pl.ds(2, 2)], s_relay.at[n], relay_sem.at[n], sib) for n, (m, size) in enumerate(NEAR + FAR)}

    starts = list(near)
    for load in loads[:8]:
        load.wait()
    pl.semaphore_wait(barrier, 7)
    for copy in near[starts[0]]:
        copy.start()
    for load in loads[8:]:
        load.wait()
    for copy in sib_copies:
        copy.start()

    eye = lax.broadcasted_iota(jnp.int32, (LANES, LANES), 0) == lax.broadcasted_iota(jnp.int32, (LANES, LANES), 1)
    for c in range(chunks):
        g, s, r = c // (2 * SUBS), (c // 2) % SUBS, (c % 2) * LANES
        lo = xs[g, s, 0, pl.ds(r, LANES), :].astype(jnp.float32)
        hi = xs[g, s, 1, pl.ds(r, LANES), :].astype(jnp.float32)
        off = jnp.sum(lo * lo + hi * hi, axis=1, keepdims=True) * sq_scale
        q_row = q_ref[c : c + 1, :]
        aux[g, s, pl.ds(c % 2, 1), :] = jnp.sum(jnp.where(eye, off, 0.0), axis=0, keepdims=True)
        aux[g, s, pl.ds(2 + c % 2, 1), :] = q_row
        q_col = jnp.sum(jnp.where(eye, q_row, 0.0), axis=1, keepdims=True)
        mag = jnp.log(jnp.abs(q_col)) * log2e
        wide = (LANES, LANES)
        host_a[pl.ds(c * LANES, LANES), :] = jnp.broadcast_to(off + mag, wide)
        host_l[pl.ds(c * LANES, LANES), :] = jnp.broadcast_to(mag, wide)
        host_s[pl.ds(c * LANES, LANES), :] = jnp.broadcast_to(jnp.where(q_col < 0.0, -1.0, 1.0), wide)
    acc[...] = jnp.zeros_like(acc)
    rsum[...] = jnp.zeros_like(rsum)
    wts[1, ...] = jnp.zeros_like(wts[1, ...])

    aux_plan = [
        (aux.at[0], aux.at[own_groups], sib),
        (aux.at[1, pl.ds(0, 2)], aux.at[first, pl.ds(2, 2)], sib),
        (aux.at[1, pl.ds(2, 2)], aux.at[last, pl.ds(0, 2)], sib),
    ]
    for h in range(2):
        at, turned = first + half * h, first + half * (1 - h)
        aux_plan += [
            (aux.at[h], aux.at[pl.ds(at, half), 0], right),
            (aux.at[h], aux.at[pl.ds(turned, half), 1], left),
            (aux.at[h], aux.at[pl.ds(at + 1, half), 2], right_x),
            (aux.at[h], aux.at[pl.ds(turned + 1, half), 3], left_x),
            (aux.at[h], aux.at[pl.ds(far, half), h], opp),
            (aux.at[h], aux.at[pl.ds(far + 1, half), 2 + h], opp_x),
        ]
    aux_copies = [remote(src, dst, s_aux.at[n], aux_sem.at[n], dev) for n, (src, dst, dev) in enumerate(aux_plan)]
    for copy in aux_copies:
        copy.start()

    def send(at):
        for copy in near.get(at) or forward[at]:
            copy.start()

    def tile(g, s):
        return jnp.concatenate([xs[g, s, 0], xs[g, s, 1]], axis=1)

    def host_tile(t):
        return jnp.concatenate([tile(t * 2 // SUBS, t * 2 % SUBS), tile((t * 2 + 1) // SUBS, (t * 2 + 1) % SUBS)], axis=0)

    def weights(t, subs, slot, diag):
        hx = host_tile(t)
        base = t * HOST
        for n, (g, s) in enumerate(subs):
            dots = lax.dot_general(hx, tile(g, s), (((1,), (1,)), ((), ())), preferred_element_type=jnp.float32)
            step = LANES if diag else HOST
            for r in range(0, HOST, step):
                at = pl.ds(base + r, step)
                off, cap, total = host_a[at, :], host_l[at, :], rsum[at, :]
                for c in range(2):
                    power = dots[r : r + step, c * LANES : (c + 1) * LANES] * dot_scale + off + aux[g, s, pl.ds(c, 1), :]
                    w = jnp.exp2(jnp.minimum(power, cap)) * aux[g, s, pl.ds(2 + c, 1), :]
                    if diag and base + r == (g * SUBS + s) * QUANT + c * LANES:
                        w = jnp.where(eye, 0.0, w)
                    total = total + w
                    wts[slot, 2 * n + c, pl.ds(r, step), :] = w.astype(jnp.bfloat16)
                rsum[at, :] = total

    def pull(t, subs, slot):
        part = None
        for n, (g, s) in enumerate(subs):
            w = jnp.concatenate([wts[slot, 2 * n], wts[slot, 2 * n + 1]], axis=1)
            d = jnp.dot(w, tile(g, s), preferred_element_type=jnp.float32)
            part = d if part is None else part + d
        acc[pl.ds(t * HOST, HOST), :] += part

    def visit(subs, before, diag=False):
        for t in range(hosts):
            if t == 0:
                pull(hosts - 1, before, 1)
            else:
                pull(t - 1, subs, (t - 1) % 2)
            weights(t, subs, t % 2, diag)

    def all_of(g):
        return [(g, s) for s in range(SUBS)]

    send(first + 1)
    visit(all_of(0), all_of(0), True)
    send(first + 2)
    visit(all_of(1), all_of(0), True)
    for copy in sib_copies + aux_copies:
        copy.wait_recv()

    def step(g, carry):
        for at in (*near, *forward):
            if at == last - 1:
                continue

            @pl.when(g == at)
            def _():
                for copy in near.get(at) or forward[at]:
                    copy.wait_recv()
                relays[at].start()

        for at in range(own_groups, last - first - 1):

            @pl.when(g == at)
            def _():
                send(first + 1 + at)

        for at, copy in relays.items():

            @pl.when(g == at + 1)
            def _():
                copy.wait_recv()

        visit(all_of(g), all_of(g - 1))
        return carry

    lax.fori_loop(own_groups, last - 1, step, 0)
    relays[last - 2].wait_recv()
    rest = [(last, 0), (last, 1), (last - 1, 2), (last - 1, 3)]
    visit(rest, all_of(last - 2))
    for copy in forward[last - 1]:
        copy.wait_recv()
    relays[last - 1].start()
    late = [(last - 1, 0), (last - 1, 1)]
    visit(late, rest)
    relays[last - 1].wait_recv()
    end = [(last, 2), (last, 3)]
    visit(end, late)
    energy = jnp.zeros((8, LANES), jnp.float32)
    for r in range(0, rows_dev, HOST):
        at = pl.ds(r, HOST)
        energy = energy + jnp.sum((rsum[at, :] * host_s[at, :]).reshape(HOST // 8, 8, LANES), axis=0)
    ebuf[me] = energy
    pull(hosts - 1, end, 1)
    e_copies = [remote(ebuf.at[me], ebuf.at[me], s_e.at[d], e_sem.at[d], (me + d) % ring) for d in range(1, ring)]
    for copy in e_copies:
        copy.start()
    for t in range(hosts):
        at = pl.ds(t * HOST, HOST)
        total = jnp.sum(rsum[at, :], axis=1, keepdims=True)
        sign = host_s[at, :] * (1.0 / feat)
        hx = host_tile(t).astype(jnp.float32)
        f_ref[at, :] = (total * hx - acc[at, :]) * jnp.concatenate([sign, sign], axis=1)

    for copies in (*near.values(), *forward.values(), sib_copies, aux_copies, relays.values()):
        for copy in copies:
            copy.wait_send()
    for copy in e_copies:
        copy.wait()
    whole = ebuf[0]
    for d in range(1, ring):
        whole = whole + ebuf[d]
    e_ref[0] = 0.5 * jnp.sum(whole)


def solution(mesh):
    ring = mesh.shape["row"]

    def device_body(pos, chg):
        rows, feat = pos.shape
        groups = ring * rows // (QUANT * SUBS)
        quanta = rows // QUANT
        assert ring == 8 and feat == 2 * LANES and quanta == 8
        dma = pltpu.SemaphoreType.DMA
        f32 = jnp.float32
        vmem = pltpu.VMEM
        scratch = [
            vmem((groups, SUBS, 2, QUANT, LANES), jnp.bfloat16),
            vmem((groups, SUBS, 4, LANES), f32),
            vmem((rows, LANES), f32),
            vmem((rows, LANES), f32),
            vmem((rows, LANES), f32),
            vmem((2, 2 * SUBS, HOST, LANES), jnp.bfloat16),
            vmem((rows, feat), f32),
            vmem((rows, LANES), f32),
            vmem((ring, 8, LANES), f32),
            dma((quanta, 2)),
        ]
        for _ in range(2):
            scratch += [dma((len(NEAR), 2)), dma((len(FAR), 2)), dma((len(NEAR + FAR),)), dma((3,)), dma((15,)), dma((ring,))]
        forces, energy = pl.pallas_call(
            functools.partial(kernel, (groups, rows, ring)),
            out_shape=(jax.ShapeDtypeStruct((rows, feat), f32), jax.ShapeDtypeStruct((1,), f32)),
            in_specs=[pl.BlockSpec(memory_space=pltpu.HBM), pl.BlockSpec(memory_space=pltpu.VMEM)],
            out_specs=(pl.BlockSpec(memory_space=pltpu.VMEM), pl.BlockSpec(memory_space=pltpu.SMEM)),
            scratch_shapes=scratch,
            compiler_params=pltpu.CompilerParams(collective_id=0, has_side_effects=True, vmem_limit_bytes=63 * 2**20 - 2**19),
            name="pair_forces",
        )(pos, chg.reshape(rows // LANES, LANES))
        return forces, energy

    return jax.shard_map(device_body, mesh=mesh, in_specs=(P(("sys", "row"), None), P(("sys", "row"))), out_specs=(P(("sys", "row"), None), P("sys")), check_vma=False)
```

```python
import functools
import math

import jax
import jax.numpy as jnp
from jax import lax
from jax.experimental import pallas as pl
from jax.experimental.pallas import tpu as pltpu
from jax.sharding import PartitionSpec as P

LANES = 128
QUANT = 256
SUBS = 4
HOST = 512


def kernel(cfg, x_ref, q_ref, f_ref, e_ref, xs, aux, host_a, host_l, host_s, wts, acc, rsum, ebuf, held, head_sem, near_sem, relay_sem, sib_sem, aux_sem, e_sem, s_head, s_near, s_relay, s_sib, s_aux, s_e):
    groups, rows_dev, ring = cfg
    feat = x_ref.shape[2]
    log2e = math.log2(math.e)
    dot_scale = 2.0 * log2e / (2.0 * feat)
    sq_scale = -log2e / (2.0 * feat)
    own_groups = rows_dev // (QUANT * SUBS)
    quanta = rows_dev // QUANT
    hosts = rows_dev // HOST
    chunks = rows_dev // LANES
    me = lax.axis_index("row")
    core = me % 2
    sib = me + 1 - 2 * core
    right = (me + 2) % ring
    left = (me + ring - 2) % ring
    right_x = (sib + 2) % ring
    left_x = (sib + ring - 2) % ring
    opp = (me + 4) % ring
    opp_x = (sib + 4) % ring

    def remote(src, dst, send, recv, dev):
        return pltpu.make_async_remote_copy(src_ref=src, dst_ref=dst, send_sem=send, recv_sem=recv, device_id={"row": dev}, device_id_type=pl.DeviceIdType.MESH)

    barrier = pltpu.get_barrier_semaphore()
    for peer in (sib, right, left, right_x, left_x, opp, opp_x):
        pl.semaphore_signal(barrier, inc=1, device_id={"row": peer}, device_id_type=pl.DeviceIdType.MESH)

    first = own_groups + 1
    half = quanta // 2
    far = first + quanta
    last = groups - 1

    def near(m):
        out = []
        for d in range(2):
            q = (m + d * half) % quanta
            out.append(remote(xs.at[q // SUBS, q % SUBS], xs.at[first + m, d], s_near.at[m, d], near_sem.at[first + m, d], (right, left)[d]))
        return out

    def forward(m):
        return [remote(xs.at[first + m - quanta, d], xs.at[first + m, d], s_near.at[m, d], near_sem.at[first + m, d], (right, left)[d]) for d in range(2)]

    def relay(g):
        return remote(xs.at[g, pl.ds(0, 2)], xs.at[g + 1, pl.ds(2, 2)], s_relay.at[g], relay_sem.at[g + 1], sib)

    def arrive(g):
        for d in range(2):
            remote(xs.at[g, d], xs.at[g, d], s_near.at[0, d], near_sem.at[g, d], me).wait_recv()

    def arrive_relay(g):
        remote(xs.at[g, pl.ds(2, 2)], xs.at[g, pl.ds(2, 2)], s_relay.at[0], relay_sem.at[g], me).wait_recv()

    head = []
    for d in range(2):
        for h in range(2):
            head.append(remote(x_ref.at[d * half, :, pl.ds(h * LANES, LANES)], xs.at[first, d, h], s_head.at[d, h], head_sem.at[d, h], (right, left)[d]))
    sib_copies = []
    for k, (q, n, g, s) in enumerate([(0, 4, own_groups, 0), (4, 2, first, 2), (6, 2, last, 0)]):
        for h in range(2):
            sib_copies.append(remote(x_ref.at[pl.ds(q, n), :, pl.ds(h * LANES, LANES)], xs.at[g, pl.ds(s, n), h], s_sib.at[k, h], sib_sem.at[k, h], sib))
    pl.semaphore_wait(barrier, 7)
    for copy in head + sib_copies:
        copy.start()
    for g in range(own_groups):
        for s in range(SUBS):
            for h in range(2):
                xs[g, s, h] = x_ref[g * SUBS + s, :, h * LANES : (h + 1) * LANES]

    eye = lax.broadcasted_iota(jnp.int32, (LANES, LANES), 0) == lax.broadcasted_iota(jnp.int32, (LANES, LANES), 1)
    for c in range(chunks):
        g, s, r = c // (2 * SUBS), (c // 2) % SUBS, (c % 2) * LANES
        lo = xs[g, s, 0, pl.ds(r, LANES), :].astype(jnp.float32)
        hi = xs[g, s, 1, pl.ds(r, LANES), :].astype(jnp.float32)
        off = jnp.sum(lo * lo + hi * hi, axis=1, keepdims=True) * sq_scale
        q_row = q_ref[c : c + 1, :]
        aux[g, s, pl.ds(c % 2, 1), :] = jnp.sum(jnp.where(eye, off, 0.0), axis=0, keepdims=True)
        aux[g, s, pl.ds(2 + c % 2, 1), :] = q_row
        q_col = jnp.sum(jnp.where(eye, q_row, 0.0), axis=1, keepdims=True)
        mag = jnp.log(jnp.abs(q_col)) * log2e
        wide = (LANES, LANES)
        host_a[pl.ds(c * LANES, LANES), :] = jnp.broadcast_to(off + mag, wide)
        host_l[pl.ds(c * LANES, LANES), :] = jnp.broadcast_to(mag, wide)
        host_s[pl.ds(c * LANES, LANES), :] = jnp.broadcast_to(jnp.where(q_col < 0.0, -1.0, 1.0), wide)

    aux_plan = [
        (aux.at[0], aux.at[own_groups], sib),
        (aux.at[1, pl.ds(0, 2)], aux.at[first, pl.ds(2, 2)], sib),
        (aux.at[1, pl.ds(2, 2)], aux.at[last, pl.ds(0, 2)], sib),
    ]
    for h in range(2):
        at, turned = first + half * h, first + half * (1 - h)
        aux_plan += [
            (aux.at[h], aux.at[pl.ds(at, half), 0], right),
            (aux.at[h], aux.at[pl.ds(turned, half), 1], left),
            (aux.at[h], aux.at[pl.ds(at + 1, half), 2], right_x),
            (aux.at[h], aux.at[pl.ds(turned + 1, half), 3], left_x),
            (aux.at[h], aux.at[pl.ds(far, half), h], opp),
            (aux.at[h], aux.at[pl.ds(far + 1, half), 2 + h], opp_x),
        ]
    aux_copies = [remote(src, dst, s_aux.at[n], aux_sem.at[n], dev) for n, (src, dst, dev) in enumerate(aux_plan)]
    def tile(g, s):
        return jnp.concatenate([xs[g, s, 0], xs[g, s, 1]], axis=1)

    def host_tile(t):
        return jnp.concatenate([tile(t * 2 // SUBS, t * 2 % SUBS), tile((t * 2 + 1) // SUBS, (t * 2 + 1) % SUBS)], axis=0)

    def dots(t, g, s):
        return lax.dot_general(host_tile(t), tile(g, s), (((1,), (1,)), ((), ())), preferred_element_type=jnp.float32)

    def emit(prod, t, n, g, s, slot, diag, fresh):
        base = t * HOST
        step = LANES if diag else HOST
        for r in range(0, HOST, step):
            at = pl.ds(base + r, step)
            off, cap = host_a[at, :], host_l[at, :]
            total = None if fresh else rsum[at, :]
            for c in range(2):
                power = prod(r, step, c) * dot_scale + off + aux[g, s, pl.ds(c, 1), :]
                w = jnp.exp2(jnp.minimum(power, cap)) * aux[g, s, pl.ds(2 + c, 1), :]
                if diag and base + r == (g * SUBS + s) * QUANT + c * LANES:
                    w = jnp.where(eye, 0.0, w)
                total = w if total is None else total + w
                wts[slot, 2 * n + c, pl.ds(r, step), :] = w.astype(jnp.bfloat16)
            rsum[at, :] = total

    def weights(t, subs, slot, diag, fresh):
        for n, (g, s) in enumerate(subs):
            p = dots(t, g, s)
            emit(lambda r, step, c: p[r : r + step, c * LANES : (c + 1) * LANES], t, n, g, s, slot, diag, fresh and n == 0)

    def hold(t, subs):
        for n, (g, s) in enumerate(subs):
            p = dots(t, g, s)
            for c in range(2):
                held[2 * n + c] = p[:, c * LANES : (c + 1) * LANES]

    def finish(t, subs, slot, diag, fresh):
        for n, (g, s) in enumerate(subs):
            emit(lambda r, step, c: held[2 * n + c, pl.ds(r, step), :], t, n, g, s, slot, diag, fresh and n == 0)

    def pull(t, subs, slot, fresh):
        part = None
        for n, (g, s) in enumerate(subs):
            w = jnp.concatenate([wts[slot, 2 * n], wts[slot, 2 * n + 1]], axis=1)
            d = jnp.dot(w, tile(g, s), preferred_element_type=jnp.float32)
            part = d if part is None else part + d
        at = pl.ds(t * HOST, HOST)
        acc[at, :] = part if fresh else acc[at, :] + part

    end_tile = hosts - 1

    def visit(subs, before, diag=False, diag_before=False, fresh=False, fresh_before=False):
        if before:
            finish(end_tile, before, 1, diag_before, fresh_before)
        for t in range(end_tile):
            weights(t, subs, t % 2, diag, fresh)
            if t == 0 and before:
                pull(end_tile, before, 1, fresh_before)
            if t > 0:
                pull(t - 1, subs, (t - 1) % 2, fresh)
        hold(end_tile, subs)
        pull(end_tile - 1, subs, (end_tile - 1) % 2, fresh)

    def all_of(g):
        return [(g, s) for s in range(SUBS)]

    def start(copies):
        for copy in copies:
            copy.start()

    start(near(1))
    visit(all_of(0), None, True, fresh=True)
    start(aux_copies + near(2))
    visit(all_of(1), all_of(0), True, True, fresh_before=True)
    start(near(3))
    for copy in sib_copies + aux_copies:
        copy.wait_recv()
    visit(all_of(2), all_of(1), False, True)

    def step(g, carry):
        @pl.when(g < quanta - 1)
        def _():
            start(near(g + 1))

        @pl.when((g >= quanta - 1) & (g < last - first - 1))
        def _():
            start(forward(g + 1))

        @pl.when(g == first)
        def _():
            for copy in head:
                copy.wait_recv()

        @pl.when(g > first)
        def _():
            arrive(g)
            arrive_relay(g)

        relay(g).start()
        visit(all_of(g), all_of(g - 1))
        return carry

    lax.fori_loop(first, last - 1, step, 0)
    arrive_relay(last - 1)
    rest = [(last, 0), (last, 1), (last - 1, 2), (last - 1, 3)]
    visit(rest, all_of(last - 2))
    arrive(last - 1)
    relay(last - 1).start()
    late = [(last - 1, 0), (last - 1, 1)]
    visit(late, rest)
    arrive_relay(last)
    end = [(last, 2), (last, 3)]
    visit(end, late)
    finish(end_tile, end, 1, False, False)
    energy = jnp.zeros((8, LANES), jnp.float32)
    for r in range(0, rows_dev, HOST):
        at = pl.ds(r, HOST)
        energy = energy + jnp.sum((rsum[at, :] * host_s[at, :]).reshape(HOST // 8, 8, LANES), axis=0)
    ebuf[me] = energy
    pull(end_tile, end, 1, False)
    e_copies = [remote(ebuf.at[me], ebuf.at[me], s_e.at[d], e_sem.at[d], (me + d) % ring) for d in range(1, ring)]
    for copy in e_copies:
        copy.start()
    for t in range(hosts):
        at = pl.ds(t * HOST, HOST)
        total = jnp.sum(rsum[at, :], axis=1, keepdims=True)
        sign = host_s[at, :] * (1.0 / feat)
        hx = host_tile(t).astype(jnp.float32)
        f_ref[at, :] = (total * hx - acc[at, :]) * jnp.concatenate([sign, sign], axis=1)

    for copy in head + sib_copies + aux_copies:
        copy.wait_send()

    def drain(g, carry):
        relay(g).wait_send()
        return carry

    def drain_near(m, carry):
        for copy in near(m):
            copy.wait_send()
        return carry

    def drain_forward(m, carry):
        for copy in forward(m):
            copy.wait_send()
        return carry

    lax.fori_loop(first, last, drain, 0)
    lax.fori_loop(1, quanta, drain_near, 0)
    lax.fori_loop(quanta, last - first, drain_forward, 0)
    for copy in e_copies:
        copy.wait()
    whole = ebuf[0]
    for d in range(1, ring):
        whole = whole + ebuf[d]
    e_ref[0] = 0.5 * jnp.sum(whole)


def solution(mesh):
    ring = mesh.shape["row"]

    def device_body(pos, chg):
        rows, feat = pos.shape
        groups = ring * rows // (QUANT * SUBS)
        quanta = rows // QUANT
        assert ring == 8 and feat == 2 * LANES and quanta == 8
        dma = pltpu.SemaphoreType.DMA
        f32 = jnp.float32
        vmem = pltpu.VMEM
        scratch = [
            vmem((groups, SUBS, 2, QUANT, LANES), jnp.bfloat16),
            vmem((groups, SUBS, 4, LANES), f32),
            vmem((rows, LANES), f32),
            vmem((rows, LANES), f32),
            vmem((rows, LANES), f32),
            vmem((2, 2 * SUBS, HOST, LANES), jnp.bfloat16),
            vmem((rows, feat), f32),
            vmem((rows, LANES), f32),
            vmem((ring, 8, LANES), f32),
            vmem((2 * SUBS, HOST, LANES), f32),
        ]
        for _ in range(2):
            scratch += [dma((2, 2)), dma((groups, 2)), dma((groups,)), dma((3, 2)), dma((15,)), dma((ring,))]
        forces, energy = pl.pallas_call(
            functools.partial(kernel, (groups, rows, ring)),
            out_shape=(jax.ShapeDtypeStruct((rows, feat), f32), jax.ShapeDtypeStruct((1,), f32)),
            in_specs=[pl.BlockSpec(memory_space=pltpu.VMEM), pl.BlockSpec(memory_space=pltpu.VMEM)],
            out_specs=(pl.BlockSpec(memory_space=pltpu.VMEM), pl.BlockSpec(memory_space=pltpu.SMEM)),
            scratch_shapes=scratch,
            compiler_params=pltpu.CompilerParams(collective_id=0, has_side_effects=True, vmem_limit_bytes=40 * 2**20),
            name="pair_forces",
        )(pos.reshape(quanta, QUANT, feat), chg.reshape(rows // LANES, LANES))
        return forces, energy

    return jax.shard_map(device_body, mesh=mesh, in_specs=(P(("sys", "row"), None), P(("sys", "row"))), out_specs=(P(("sys", "row"), None), P("sys")), check_vma=False)
```

```python
import functools
import math

import jax
import jax.numpy as jnp
from jax import lax
from jax.experimental import pallas as pl
from jax.experimental.pallas import tpu as pltpu
from jax.sharding import PartitionSpec as P

LANES = 128
QUANT = 256
SUBS = 4
HOST = 512


def kernel(cfg, x_ref, q_ref, f_ref, e_ref, xs, aux, host_a, host_l, host_s, wts, acc, rsum, ebuf, head_sem, near_sem, relay_sem, sib_sem, aux_sem, e_sem, s_head, s_near, s_relay, s_sib, s_aux, s_e):
    groups, rows_dev, ring = cfg
    feat = x_ref.shape[2]
    log2e = math.log2(math.e)
    dot_scale = 2.0 * log2e / (2.0 * feat)
    sq_scale = -log2e / (2.0 * feat)
    own_groups = rows_dev // (QUANT * SUBS)
    quanta = rows_dev // QUANT
    hosts = rows_dev // HOST
    chunks = rows_dev // LANES
    me = lax.axis_index("row")
    core = me % 2
    sib = me + 1 - 2 * core
    right = (me + 2) % ring
    left = (me + ring - 2) % ring
    right_x = (sib + 2) % ring
    left_x = (sib + ring - 2) % ring
    opp = (me + 4) % ring
    opp_x = (sib + 4) % ring

    def remote(src, dst, send, recv, dev):
        return pltpu.make_async_remote_copy(src_ref=src, dst_ref=dst, send_sem=send, recv_sem=recv, device_id={"row": dev}, device_id_type=pl.DeviceIdType.MESH)

    barrier = pltpu.get_barrier_semaphore()
    for peer in (sib, right, left, right_x, left_x, opp, opp_x):
        pl.semaphore_signal(barrier, inc=1, device_id={"row": peer}, device_id_type=pl.DeviceIdType.MESH)

    first = own_groups + 1
    half = quanta // 2
    far = first + quanta
    last = groups - 1

    def near(m):
        out = []
        for d in range(2):
            q = (m + d * half) % quanta
            out.append(remote(xs.at[q // SUBS, q % SUBS], xs.at[first + m, d], s_near.at[m, d], near_sem.at[first + m, d], (right, left)[d]))
        return out

    def forward(m):
        return [remote(xs.at[first + m - quanta, d], xs.at[first + m, d], s_near.at[m, d], near_sem.at[first + m, d], (right, left)[d]) for d in range(2)]

    def relay(g):
        return remote(xs.at[g, pl.ds(0, 2)], xs.at[g + 1, pl.ds(2, 2)], s_relay.at[g], relay_sem.at[g + 1], sib)

    def arrive(g):
        for d in range(2):
            remote(xs.at[g, d], xs.at[g, d], s_near.at[0, d], near_sem.at[g, d], me).wait_recv()

    def arrive_relay(g):
        remote(xs.at[g, pl.ds(2, 2)], xs.at[g, pl.ds(2, 2)], s_relay.at[0], relay_sem.at[g], me).wait_recv()

    head = []
    for d in range(2):
        for h in range(2):
            head.append(remote(x_ref.at[d * half, :, pl.ds(h * LANES, LANES)], xs.at[first, d, h], s_head.at[d, h], head_sem.at[d, h], (right, left)[d]))
    sib_copies = []
    for k, (q, n, g, s) in enumerate([(0, 4, own_groups, 0), (4, 2, first, 2), (6, 2, last, 0)]):
        for h in range(2):
            sib_copies.append(remote(x_ref.at[pl.ds(q, n), :, pl.ds(h * LANES, LANES)], xs.at[g, pl.ds(s, n), h], s_sib.at[k, h], sib_sem.at[k, h], sib))
    pl.semaphore_wait(barrier, 7)
    for copy in head + sib_copies:
        copy.start()
    for g in range(own_groups):
        for s in range(SUBS):
            for h in range(2):
                xs[g, s, h] = x_ref[g * SUBS + s, :, h * LANES : (h + 1) * LANES]

    eye = lax.broadcasted_iota(jnp.int32, (LANES, LANES), 0) == lax.broadcasted_iota(jnp.int32, (LANES, LANES), 1)
    for c in range(chunks):
        g, s, r = c // (2 * SUBS), (c // 2) % SUBS, (c % 2) * LANES
        lo = xs[g, s, 0, pl.ds(r, LANES), :].astype(jnp.float32)
        hi = xs[g, s, 1, pl.ds(r, LANES), :].astype(jnp.float32)
        off = jnp.sum(lo * lo + hi * hi, axis=1, keepdims=True) * sq_scale
        q_row = q_ref[c : c + 1, :]
        aux[g, s, pl.ds(c % 2, 1), :] = jnp.sum(jnp.where(eye, off, 0.0), axis=0, keepdims=True)
        aux[g, s, pl.ds(2 + c % 2, 1), :] = q_row
        q_col = jnp.sum(jnp.where(eye, q_row, 0.0), axis=1, keepdims=True)
        mag = jnp.log(jnp.abs(q_col)) * log2e
        wide = (LANES, LANES)
        host_a[pl.ds(c * LANES, LANES), :] = jnp.broadcast_to(off + mag, wide)
        host_l[pl.ds(c * LANES, LANES), :] = jnp.broadcast_to(mag, wide)
        host_s[pl.ds(c * LANES, LANES), :] = jnp.broadcast_to(jnp.where(q_col < 0.0, -1.0, 1.0), wide)

    aux_plan = [
        (aux.at[0], aux.at[own_groups], sib),
        (aux.at[1, pl.ds(0, 2)], aux.at[first, pl.ds(2, 2)], sib),
        (aux.at[1, pl.ds(2, 2)], aux.at[last, pl.ds(0, 2)], sib),
    ]
    for h in range(2):
        at, turned = first + half * h, first + half * (1 - h)
        aux_plan += [
            (aux.at[h], aux.at[pl.ds(at, half), 0], right),
            (aux.at[h], aux.at[pl.ds(turned, half), 1], left),
            (aux.at[h], aux.at[pl.ds(at + 1, half), 2], right_x),
            (aux.at[h], aux.at[pl.ds(turned + 1, half), 3], left_x),
            (aux.at[h], aux.at[pl.ds(far, half), h], opp),
            (aux.at[h], aux.at[pl.ds(far + 1, half), 2 + h], opp_x),
        ]
    aux_copies = [remote(src, dst, s_aux.at[n], aux_sem.at[n], dev) for n, (src, dst, dev) in enumerate(aux_plan)]
    def tile(g, s):
        return jnp.concatenate([xs[g, s, 0], xs[g, s, 1]], axis=1)

    def host_tile(t):
        return jnp.concatenate([tile(t * 2 // SUBS, t * 2 % SUBS), tile((t * 2 + 1) // SUBS, (t * 2 + 1) % SUBS)], axis=0)

    def dots(t, g, s):
        return lax.dot_general(host_tile(t), tile(g, s), (((1,), (1,)), ((), ())), preferred_element_type=jnp.float32)

    def emit(prod, t, n, g, s, slot, diag, fresh):
        base = t * HOST
        step = LANES if diag else HOST
        for r in range(0, HOST, step):
            at = pl.ds(base + r, step)
            off, cap = host_a[at, :], host_l[at, :]
            total = None if fresh else rsum[at, :]
            for c in range(2):
                power = prod(r, step, c) * dot_scale + off + aux[g, s, pl.ds(c, 1), :]
                w = jnp.exp2(jnp.minimum(power, cap)) * aux[g, s, pl.ds(2 + c, 1), :]
                if diag and base + r == (g * SUBS + s) * QUANT + c * LANES:
                    w = jnp.where(eye, 0.0, w)
                total = w if total is None else total + w
                wts[slot, 2 * n + c, pl.ds(r, step), :] = w.astype(jnp.bfloat16)
            rsum[at, :] = total

    def weights(t, subs, slot, diag, fresh):
        for n, (g, s) in enumerate(subs):
            p = dots(t, g, s)
            emit(lambda r, step, c: p[r : r + step, c * LANES : (c + 1) * LANES], t, n, g, s, slot, diag, fresh and n == 0)

    def pull(t, subs, slot, fresh):
        part = None
        for n, (g, s) in enumerate(subs):
            w = jnp.concatenate([wts[slot, 2 * n], wts[slot, 2 * n + 1]], axis=1)
            d = jnp.dot(w, tile(g, s), preferred_element_type=jnp.float32)
            part = d if part is None else part + d
        at = pl.ds(t * HOST, HOST)
        acc[at, :] = part if fresh else acc[at, :] + part

    end_tile = hosts - 1

    def visit(subs, before, diag=False, fresh=False, fresh_before=False):
        for t in range(hosts):
            if t > 0:
                pull(t - 1, subs, (t - 1) % 2, fresh)
            elif before:
                pull(end_tile, before, 1, fresh_before)
            weights(t, subs, t % 2, diag, fresh)

    def all_of(g):
        return [(g, s) for s in range(SUBS)]

    def start(copies):
        for copy in copies:
            copy.start()

    start(near(1))
    visit(all_of(0), None, True, fresh=True)
    start(aux_copies + near(2))
    visit(all_of(1), all_of(0), True, fresh_before=True)
    for copy in sib_copies + aux_copies:
        copy.wait_recv()

    def step(g, carry):
        @pl.when(g < quanta - 1)
        def _():
            start(near(g + 1))

        @pl.when((g >= quanta - 1) & (g < last - first - 1))
        def _():
            start(forward(g + 1))

        @pl.when(g == first)
        def _():
            for copy in head:
                copy.wait_recv()

        @pl.when(g > first)
        def _():
            arrive(g)
            arrive_relay(g)

        @pl.when(g >= first)
        def _():
            relay(g).start()

        visit(all_of(g), all_of(g - 1))
        return carry

    lax.fori_loop(own_groups, last - 1, step, 0)
    arrive_relay(last - 1)
    rest = [(last, 0), (last, 1), (last - 1, 2), (last - 1, 3)]
    visit(rest, all_of(last - 2))
    arrive(last - 1)
    relay(last - 1).start()
    late = [(last - 1, 0), (last - 1, 1)]
    visit(late, rest)
    arrive_relay(last)
    end = [(last, 2), (last, 3)]
    visit(end, late)
    energy = jnp.zeros((8, LANES), jnp.float32)
    for r in range(0, rows_dev, HOST):
        at = pl.ds(r, HOST)
        energy = energy + jnp.sum((rsum[at, :] * host_s[at, :]).reshape(HOST // 8, 8, LANES), axis=0)
    ebuf[me] = energy
    pull(end_tile, end, 1, False)
    e_copies = [remote(ebuf.at[me], ebuf.at[me], s_e.at[d], e_sem.at[d], (me + d) % ring) for d in range(1, ring)]
    for copy in e_copies:
        copy.start()
    for t in range(hosts):
        at = pl.ds(t * HOST, HOST)
        total = jnp.sum(rsum[at, :], axis=1, keepdims=True)
        sign = host_s[at, :] * (1.0 / feat)
        hx = host_tile(t).astype(jnp.float32)
        f_ref[at, :] = (total * hx - acc[at, :]) * jnp.concatenate([sign, sign], axis=1)

    for copy in head + sib_copies + aux_copies:
        copy.wait_send()

    def drain(g, carry):
        relay(g).wait_send()
        return carry

    def drain_near(m, carry):
        for copy in near(m):
            copy.wait_send()
        return carry

    def drain_forward(m, carry):
        for copy in forward(m):
            copy.wait_send()
        return carry

    lax.fori_loop(first, last, drain, 0)
    lax.fori_loop(1, quanta, drain_near, 0)
    lax.fori_loop(quanta, last - first, drain_forward, 0)
    for copy in e_copies:
        copy.wait()
    whole = ebuf[0]
    for d in range(1, ring):
        whole = whole + ebuf[d]
    e_ref[0] = 0.5 * jnp.sum(whole)


def solution(mesh):
    ring = mesh.shape["row"]

    def device_body(pos, chg):
        rows, feat = pos.shape
        groups = ring * rows // (QUANT * SUBS)
        quanta = rows // QUANT
        assert ring == 8 and feat == 2 * LANES and quanta == 8
        dma = pltpu.SemaphoreType.DMA
        f32 = jnp.float32
        vmem = pltpu.VMEM
        scratch = [
            vmem((groups, SUBS, 2, QUANT, LANES), jnp.bfloat16),
            vmem((groups, SUBS, 4, LANES), f32),
            vmem((rows, LANES), f32),
            vmem((rows, LANES), f32),
            vmem((rows, LANES), f32),
            vmem((2, 2 * SUBS, HOST, LANES), jnp.bfloat16),
            vmem((rows, feat), f32),
            vmem((rows, LANES), f32),
            vmem((ring, 8, LANES), f32),
        ]
        for _ in range(2):
            scratch += [dma((2, 2)), dma((groups, 2)), dma((groups,)), dma((3, 2)), dma((15,)), dma((ring,))]
        forces, energy = pl.pallas_call(
            functools.partial(kernel, (groups, rows, ring)),
            out_shape=(jax.ShapeDtypeStruct((rows, feat), f32), jax.ShapeDtypeStruct((1,), f32)),
            in_specs=[pl.BlockSpec(memory_space=pltpu.VMEM), pl.BlockSpec(memory_space=pltpu.VMEM)],
            out_specs=(pl.BlockSpec(memory_space=pltpu.VMEM), pl.BlockSpec(memory_space=pltpu.SMEM)),
            scratch_shapes=scratch,
            compiler_params=pltpu.CompilerParams(collective_id=0, has_side_effects=True, vmem_limit_bytes=40 * 2**20),
            name="pair_forces",
        )(pos.reshape(quanta, QUANT, feat), chg.reshape(rows // LANES, LANES))
        return forces, energy

    return jax.shard_map(device_body, mesh=mesh, in_specs=(P(("sys", "row"), None), P(("sys", "row"))), out_specs=(P(("sys", "row"), None), P("sys")), check_vma=False)
```

```python
import functools
import math

import jax
import jax.numpy as jnp
from jax import lax
from jax.experimental import pallas as pl
from jax.experimental.pallas import tpu as pltpu
from jax.sharding import PartitionSpec as P

LANES = 128
QUANT = 256
SUBS = 4
HOST = 512


def kernel(cfg, x_ref, q_ref, f_ref, e_ref, xs, aux, host_a, host_l, host_s, wts, acc, rsum, ebuf, head_sem, near_sem, relay_sem, sib_sem, aux_sem, e_sem, s_head, s_near, s_relay, s_sib, s_aux, s_e):
    groups, rows_dev, ring = cfg
    feat = x_ref.shape[2]
    log2e = math.log2(math.e)
    dot_scale = 2.0 * log2e / (2.0 * feat)
    sq_scale = -log2e / (2.0 * feat)
    own_groups = rows_dev // (QUANT * SUBS)
    quanta = rows_dev // QUANT
    hosts = rows_dev // HOST
    chunks = rows_dev // LANES
    me = lax.axis_index("row")
    core = me % 2
    sib = me + 1 - 2 * core
    right = (me + 2) % ring
    left = (me + ring - 2) % ring
    right_x = (sib + 2) % ring
    left_x = (sib + ring - 2) % ring
    opp = (me + 4) % ring
    opp_x = (sib + 4) % ring

    def remote(src, dst, send, recv, dev):
        return pltpu.make_async_remote_copy(src_ref=src, dst_ref=dst, send_sem=send, recv_sem=recv, device_id={"row": dev}, device_id_type=pl.DeviceIdType.MESH)

    barrier = pltpu.get_barrier_semaphore()
    for peer in (sib, right, left, right_x, left_x, opp, opp_x):
        pl.semaphore_signal(barrier, inc=1, device_id={"row": peer}, device_id_type=pl.DeviceIdType.MESH)

    first = own_groups + 1
    half = quanta // 2
    far = first + quanta
    last = groups - 1

    def hop(m, turn):
        d = (core + turn) % 2
        on = m // quanta
        src = (1 - on) * ((m + d * half) % quanta) + on * ((first + m - quanta) * SUBS + d)
        dst = (first + m) * SUBS + d
        return remote(xs.at[src], xs.at[dst], s_near.at[m, d], near_sem.at[first + m, d], (me + 2 + d * (ring - 4)) % ring)

    def hop_first(turn):
        d = (core + turn) % 2
        return [remote(x_ref.at[d * half, :, pl.ds(h * LANES, LANES)], xs.at[first * SUBS + d, h], s_head.at[d, h], head_sem.at[d, h], (me + 2 + d * (ring - 4)) % ring) for h in range(2)]

    def relay(g):
        return remote(xs.at[pl.ds(g * SUBS, 2)], xs.at[pl.ds((g + 1) * SUBS + 2, 2)], s_relay.at[g], relay_sem.at[g + 1], sib)

    def arrive(g):
        for d in range(2):
            remote(xs.at[g * SUBS + d], xs.at[g * SUBS + d], s_near.at[0, d], near_sem.at[g, d], me).wait_recv()

    def arrive_relay(g):
        at = pl.ds(g * SUBS + 2, 2)
        remote(xs.at[at], xs.at[at], s_relay.at[0], relay_sem.at[g], me).wait_recv()

    sib_copies = []
    for k, (q, n, at) in enumerate([(0, 4, own_groups * SUBS), (4, 2, first * SUBS + 2), (6, 2, last * SUBS)]):
        for h in range(2):
            sib_copies.append(remote(x_ref.at[pl.ds(q, n), :, pl.ds(h * LANES, LANES)], xs.at[pl.ds(at, n), h], s_sib.at[k, h], sib_sem.at[k, h], sib))
    head = hop_first(0) + hop_first(1)
    pl.semaphore_wait(barrier, 7)
    for copy in head[:2] + sib_copies:
        copy.start()
    for g in range(own_groups):
        for s in range(SUBS):
            for h in range(2):
                xs[g * SUBS + s, h] = x_ref[g * SUBS + s, :, h * LANES : (h + 1) * LANES]

    eye = lax.broadcasted_iota(jnp.int32, (LANES, LANES), 0) == lax.broadcasted_iota(jnp.int32, (LANES, LANES), 1)
    for c in range(chunks):
        g, s, r = c // (2 * SUBS), (c // 2) % SUBS, (c % 2) * LANES
        lo = xs[g * SUBS + s, 0, pl.ds(r, LANES), :].astype(jnp.float32)
        hi = xs[g * SUBS + s, 1, pl.ds(r, LANES), :].astype(jnp.float32)
        off = jnp.sum(lo * lo + hi * hi, axis=1, keepdims=True) * sq_scale
        q_row = q_ref[c : c + 1, :]
        aux[g, s, pl.ds(c % 2, 1), :] = jnp.sum(jnp.where(eye, off, 0.0), axis=0, keepdims=True)
        aux[g, s, pl.ds(2 + c % 2, 1), :] = q_row
        q_col = jnp.sum(jnp.where(eye, q_row, 0.0), axis=1, keepdims=True)
        mag = jnp.log(jnp.abs(q_col)) * log2e
        wide = (LANES, LANES)
        host_a[pl.ds(c * LANES, LANES), :] = jnp.broadcast_to(off + mag, wide)
        host_l[pl.ds(c * LANES, LANES), :] = jnp.broadcast_to(mag, wide)
        host_s[pl.ds(c * LANES, LANES), :] = jnp.broadcast_to(jnp.where(q_col < 0.0, -1.0, 1.0), wide)

    aux_plan = [
        (aux.at[0], aux.at[own_groups], sib),
        (aux.at[1, pl.ds(0, 2)], aux.at[first, pl.ds(2, 2)], sib),
        (aux.at[1, pl.ds(2, 2)], aux.at[last, pl.ds(0, 2)], sib),
    ]
    for h in range(2):
        at, turned = first + half * h, first + half * (1 - h)
        aux_plan += [
            (aux.at[h], aux.at[pl.ds(at, half), 0], right),
            (aux.at[h], aux.at[pl.ds(turned, half), 1], left),
            (aux.at[h], aux.at[pl.ds(at + 1, half), 2], right_x),
            (aux.at[h], aux.at[pl.ds(turned + 1, half), 3], left_x),
            (aux.at[h], aux.at[pl.ds(far, half), h], opp),
            (aux.at[h], aux.at[pl.ds(far + 1, half), 2 + h], opp_x),
        ]
    aux_copies = [remote(src, dst, s_aux.at[n], aux_sem.at[n], dev) for n, (src, dst, dev) in enumerate(aux_plan)]
    def tile(g, s):
        return jnp.concatenate([xs[g * SUBS + s, 0], xs[g * SUBS + s, 1]], axis=1)

    def host_tile(t):
        return jnp.concatenate([tile(t * 2 // SUBS, t * 2 % SUBS), tile((t * 2 + 1) // SUBS, (t * 2 + 1) % SUBS)], axis=0)

    def dots(t, g, s):
        return lax.dot_general(host_tile(t), tile(g, s), (((1,), (1,)), ((), ())), preferred_element_type=jnp.float32)

    def emit(prod, t, n, g, s, slot, diag, fresh):
        base = t * HOST
        step = LANES if diag else HOST
        for r in range(0, HOST, step):
            at = pl.ds(base + r, step)
            off, cap = host_a[at, :], host_l[at, :]
            total = None if fresh else rsum[at, :]
            for c in range(2):
                power = prod(r, step, c) * dot_scale + off + aux[g, s, pl.ds(c, 1), :]
                w = jnp.exp2(jnp.minimum(power, cap)) * aux[g, s, pl.ds(2 + c, 1), :]
                if diag and base + r == (g * SUBS + s) * QUANT + c * LANES:
                    w = jnp.where(eye, 0.0, w)
                total = w if total is None else total + w
                wts[slot, 2 * n + c, pl.ds(r, step), :] = w.astype(jnp.bfloat16)
            rsum[at, :] = total

    def weights(t, subs, slot, diag, fresh):
        for n, (g, s) in enumerate(subs):
            p = dots(t, g, s)
            emit(lambda r, step, c: p[r : r + step, c * LANES : (c + 1) * LANES], t, n, g, s, slot, diag, fresh and n == 0)

    def pull(t, subs, slot, fresh):
        part = None
        for n, (g, s) in enumerate(subs):
            w = jnp.concatenate([wts[slot, 2 * n], wts[slot, 2 * n + 1]], axis=1)
            d = jnp.dot(w, tile(g, s), preferred_element_type=jnp.float32)
            part = d if part is None else part + d
        at = pl.ds(t * HOST, HOST)
        acc[at, :] = part if fresh else acc[at, :] + part

    end_tile = hosts - 1

    def visit(subs, before, diag=False, fresh=False, fresh_before=False, sends=None):
        for t in range(hosts):
            if t > 0:
                pull(t - 1, subs, (t - 1) % 2, fresh)
            elif before:
                pull(end_tile, before, 1, fresh_before)
            weights(t, subs, t % 2, diag, fresh)
            if sends is not None and t == hosts // 2 - 1:
                hop(sends, 1).start()

    def all_of(g):
        return [(g, s) for s in range(SUBS)]

    def start(copies):
        for copy in copies:
            copy.start()

    start(head[2:] + [hop(1, 0)])
    visit(all_of(0), None, True, fresh=True, sends=1)
    start(aux_copies + [hop(2, 0)])
    visit(all_of(1), all_of(0), True, fresh_before=True, sends=2)
    for copy in sib_copies + aux_copies:
        copy.wait_recv()

    def step(g, carry):
        m = g + 1
        for turn in range(2):
            hop(m - 2, turn).wait_send()
        hop(m, 0).start()

        @pl.when(g == first)
        def _():
            for copy in head:
                copy.wait_recv()

        @pl.when(g > first)
        def _():
            arrive(g)
            arrive_relay(g)

        @pl.when(g >= first)
        def _():
            relay(g).start()

        visit(all_of(g), all_of(g - 1), sends=m)
        return carry

    sends_end = last - first - 1
    lax.fori_loop(own_groups, sends_end, step, 0)

    def step_late(g, carry):
        arrive(g)
        arrive_relay(g)
        relay(g).start()
        visit(all_of(g), all_of(g - 1))
        return carry

    lax.fori_loop(sends_end, last - 1, step_late, 0)
    arrive_relay(last - 1)
    rest = [(last, 0), (last, 1), (last - 1, 2), (last - 1, 3)]
    visit(rest, all_of(last - 2))
    arrive(last - 1)
    relay(last - 1).start()
    late = [(last - 1, 0), (last - 1, 1)]
    visit(late, rest)
    arrive_relay(last)
    end = [(last, 2), (last, 3)]
    visit(end, late)
    energy = jnp.zeros((8, LANES), jnp.float32)
    for r in range(0, rows_dev, HOST):
        at = pl.ds(r, HOST)
        energy = energy + jnp.sum((rsum[at, :] * host_s[at, :]).reshape(HOST // 8, 8, LANES), axis=0)
    ebuf[me] = energy
    pull(end_tile, end, 1, False)
    e_copies = [remote(ebuf.at[me], ebuf.at[me], s_e.at[d], e_sem.at[d], (me + d) % ring) for d in range(1, ring)]
    for copy in e_copies:
        copy.start()
    for t in range(hosts):
        at = pl.ds(t * HOST, HOST)
        total = jnp.sum(rsum[at, :], axis=1, keepdims=True)
        sign = host_s[at, :] * (1.0 / feat)
        hx = host_tile(t).astype(jnp.float32)
        f_ref[at, :] = (total * hx - acc[at, :]) * jnp.concatenate([sign, sign], axis=1)

    for copy in head + sib_copies + aux_copies:
        copy.wait_send()

    def drain(g, carry):
        relay(g).wait_send()
        return carry

    lax.fori_loop(first, last, drain, 0)
    for m in range(sends_end - 1, sends_end + 1):
        for turn in range(2):
            hop(m, turn).wait_send()
    for copy in e_copies:
        copy.wait()
    whole = ebuf[0]
    for d in range(1, ring):
        whole = whole + ebuf[d]
    e_ref[0] = 0.5 * jnp.sum(whole)


def solution(mesh):
    ring = mesh.shape["row"]

    def device_body(pos, chg):
        rows, feat = pos.shape
        groups = ring * rows // (QUANT * SUBS)
        quanta = rows // QUANT
        assert ring == 8 and feat == 2 * LANES and quanta == 8
        dma = pltpu.SemaphoreType.DMA
        f32 = jnp.float32
        vmem = pltpu.VMEM
        scratch = [
            vmem((groups * SUBS, 2, QUANT, LANES), jnp.bfloat16),
            vmem((groups, SUBS, 4, LANES), f32),
            vmem((rows, LANES), f32),
            vmem((rows, LANES), f32),
            vmem((rows, LANES), f32),
            vmem((2, 2 * SUBS, HOST, LANES), jnp.bfloat16),
            vmem((rows, feat), f32),
            vmem((rows, LANES), f32),
            vmem((ring, 8, LANES), f32),
        ]
        for _ in range(2):
            scratch += [dma((2, 2)), dma((groups, 2)), dma((groups,)), dma((3, 2)), dma((15,)), dma((ring,))]
        forces, energy = pl.pallas_call(
            functools.partial(kernel, (groups, rows, ring)),
            out_shape=(jax.ShapeDtypeStruct((rows, feat), f32), jax.ShapeDtypeStruct((1,), f32)),
            in_specs=[pl.BlockSpec(memory_space=pltpu.VMEM), pl.BlockSpec(memory_space=pltpu.VMEM)],
            out_specs=(pl.BlockSpec(memory_space=pltpu.VMEM), pl.BlockSpec(memory_space=pltpu.SMEM)),
            scratch_shapes=scratch,
            compiler_params=pltpu.CompilerParams(collective_id=0, has_side_effects=True, vmem_limit_bytes=40 * 2**20),
            name="pair_forces",
        )(pos.reshape(quanta, QUANT, feat), chg.reshape(rows // LANES, LANES))
        return forces, energy

    return jax.shard_map(device_body, mesh=mesh, in_specs=(P(("sys", "row"), None), P(("sys", "row"))), out_specs=(P(("sys", "row"), None), P("sys")), check_vma=False)
```

```python
import functools
import math

import jax
import jax.numpy as jnp
from jax import lax
from jax.experimental import pallas as pl
from jax.experimental.pallas import tpu as pltpu
from jax.sharding import PartitionSpec as P

LANES = 128
QUANT = 256
SUBS = 4
HOST = 512


def kernel(cfg, x_ref, q_ref, f_ref, e_ref, xs, aux, host_a, host_l, host_s, wts, acc, rsum, ebuf, head_sem, near_sem, relay_sem, sib_sem, aux_sem, e_sem, s_head, s_near, s_relay, s_sib, s_aux, s_e):
    groups, rows_dev, ring = cfg
    feat = x_ref.shape[2]
    log2e = math.log2(math.e)
    dot_scale = 2.0 * log2e / (2.0 * feat)
    sq_scale = -log2e / (2.0 * feat)
    own_groups = rows_dev // (QUANT * SUBS)
    quanta = rows_dev // QUANT
    hosts = rows_dev // HOST
    chunks = rows_dev // LANES
    me = lax.axis_index("row")
    core = me % 2
    sib = me + 1 - 2 * core
    right = (me + 2) % ring
    left = (me + ring - 2) % ring
    right_x = (sib + 2) % ring
    left_x = (sib + ring - 2) % ring
    opp = (me + 4) % ring
    opp_x = (sib + 4) % ring

    def remote(src, dst, send, recv, dev):
        return pltpu.make_async_remote_copy(src_ref=src, dst_ref=dst, send_sem=send, recv_sem=recv, device_id={"row": dev}, device_id_type=pl.DeviceIdType.MESH)

    barrier = pltpu.get_barrier_semaphore()
    for peer in (sib, right, left, right_x, left_x, opp, opp_x):
        pl.semaphore_signal(barrier, inc=1, device_id={"row": peer}, device_id_type=pl.DeviceIdType.MESH)

    first = own_groups + 1
    half = quanta // 2
    far = first + quanta
    last = groups - 1

    def hop(m, turn):
        d = (core + turn) % 2
        on = m // quanta
        src = (1 - on) * ((m + d * half) % quanta) + on * ((first + m - quanta) * SUBS + d)
        dst = (first + m) * SUBS + d
        return remote(xs.at[src], xs.at[dst], s_near.at[m, d], near_sem.at[first + m, d], (me + 2 + d * (ring - 4)) % ring)

    def hop_first(turn):
        d = (core + turn) % 2
        return [remote(x_ref.at[d * half, :, pl.ds(h * LANES, LANES)], xs.at[first * SUBS + d, h], s_head.at[d, h], head_sem.at[d, h], (me + 2 + d * (ring - 4)) % ring) for h in range(2)]

    def relay(g):
        return remote(xs.at[pl.ds(g * SUBS, 2)], xs.at[pl.ds((g + 1) * SUBS + 2, 2)], s_relay.at[g], relay_sem.at[g + 1], sib)

    def arrive(g):
        for d in range(2):
            remote(xs.at[g * SUBS + d], xs.at[g * SUBS + d], s_near.at[0, d], near_sem.at[g, d], me).wait_recv()

    def arrive_relay(g):
        at = pl.ds(g * SUBS + 2, 2)
        remote(xs.at[at], xs.at[at], s_relay.at[0], relay_sem.at[g], me).wait_recv()

    sib_copies = []
    for k, (q, n, at) in enumerate([(0, 4, own_groups * SUBS), (4, 2, first * SUBS + 2), (6, 2, last * SUBS)]):
        for h in range(2):
            sib_copies.append(remote(x_ref.at[pl.ds(q, n), :, pl.ds(h * LANES, LANES)], xs.at[pl.ds(at, n), h], s_sib.at[k, h], sib_sem.at[k, h], sib))
    head = hop_first(0) + hop_first(1)
    pl.semaphore_wait(barrier, 7)
    for copy in head + sib_copies:
        copy.start()
    for g in range(own_groups):
        for s in range(SUBS):
            for h in range(2):
                xs[g * SUBS + s, h] = x_ref[g * SUBS + s, :, h * LANES : (h + 1) * LANES]

    eye = lax.broadcasted_iota(jnp.int32, (LANES, LANES), 0) == lax.broadcasted_iota(jnp.int32, (LANES, LANES), 1)
    for c in range(chunks):
        g, s, r = c // (2 * SUBS), (c // 2) % SUBS, (c % 2) * LANES
        lo = xs[g * SUBS + s, 0, pl.ds(r, LANES), :].astype(jnp.float32)
        hi = xs[g * SUBS + s, 1, pl.ds(r, LANES), :].astype(jnp.float32)
        off = jnp.sum(lo * lo + hi * hi, axis=1, keepdims=True) * sq_scale
        q_row = q_ref[c : c + 1, :]
        aux[g, s, pl.ds(c % 2, 1), :] = jnp.sum(jnp.where(eye, off, 0.0), axis=0, keepdims=True)
        aux[g, s, pl.ds(2 + c % 2, 1), :] = q_row
        q_col = jnp.sum(jnp.where(eye, q_row, 0.0), axis=1, keepdims=True)
        mag = jnp.log(jnp.abs(q_col)) * log2e
        wide = (LANES, LANES)
        host_a[pl.ds(c * LANES, LANES), :] = jnp.broadcast_to(off + mag, wide)
        host_l[pl.ds(c * LANES, LANES), :] = jnp.broadcast_to(mag, wide)
        host_s[pl.ds(c * LANES, LANES), :] = jnp.broadcast_to(jnp.where(q_col < 0.0, -1.0, 1.0), wide)

    aux_plan = [
        (aux.at[0], aux.at[own_groups], sib),
        (aux.at[1, pl.ds(0, 2)], aux.at[first, pl.ds(2, 2)], sib),
        (aux.at[1, pl.ds(2, 2)], aux.at[last, pl.ds(0, 2)], sib),
    ]
    for h in range(2):
        at, turned = first + half * h, first + half * (1 - h)
        aux_plan += [
            (aux.at[h], aux.at[pl.ds(at, half), 0], right),
            (aux.at[h], aux.at[pl.ds(turned, half), 1], left),
            (aux.at[h], aux.at[pl.ds(at + 1, half), 2], right_x),
            (aux.at[h], aux.at[pl.ds(turned + 1, half), 3], left_x),
            (aux.at[h], aux.at[pl.ds(far, half), h], opp),
            (aux.at[h], aux.at[pl.ds(far + 1, half), 2 + h], opp_x),
        ]
    aux_copies = [remote(src, dst, s_aux.at[n], aux_sem.at[n], dev) for n, (src, dst, dev) in enumerate(aux_plan)]
    def tile(g, s):
        return jnp.concatenate([xs[g * SUBS + s, 0], xs[g * SUBS + s, 1]], axis=1)

    def host_tile(t):
        return jnp.concatenate([tile(t * 2 // SUBS, t * 2 % SUBS), tile((t * 2 + 1) // SUBS, (t * 2 + 1) % SUBS)], axis=0)

    def dots(t, g, s):
        return lax.dot_general(host_tile(t), tile(g, s), (((1,), (1,)), ((), ())), preferred_element_type=jnp.float32)

    def emit(prod, t, n, g, s, slot, diag, fresh):
        base = t * HOST
        step = LANES if diag else HOST
        for r in range(0, HOST, step):
            at = pl.ds(base + r, step)
            off, cap = host_a[at, :], host_l[at, :]
            total = None if fresh else rsum[at, :]
            for c in range(2):
                power = prod(r, step, c) * dot_scale + off + aux[g, s, pl.ds(c, 1), :]
                w = jnp.exp2(jnp.minimum(power, cap)) * aux[g, s, pl.ds(2 + c, 1), :]
                if diag and base + r == (g * SUBS + s) * QUANT + c * LANES:
                    w = jnp.where(eye, 0.0, w)
                total = w if total is None else total + w
                wts[slot, 2 * n + c, pl.ds(r, step), :] = w.astype(jnp.bfloat16)
            rsum[at, :] = total

    def weights(t, subs, slot, diag, fresh):
        for n, (g, s) in enumerate(subs):
            p = dots(t, g, s)
            emit(lambda r, step, c: p[r : r + step, c * LANES : (c + 1) * LANES], t, n, g, s, slot, diag, fresh and n == 0)

    def pull(t, subs, slot, fresh):
        part = None
        for n, (g, s) in enumerate(subs):
            w = jnp.concatenate([wts[slot, 2 * n], wts[slot, 2 * n + 1]], axis=1)
            d = jnp.dot(w, tile(g, s), preferred_element_type=jnp.float32)
            part = d if part is None else part + d
        at = pl.ds(t * HOST, HOST)
        acc[at, :] = part if fresh else acc[at, :] + part

    end_tile = hosts - 1

    def visit(subs, before, diag=False, fresh=False, fresh_before=False):
        for t in range(hosts):
            if t > 0:
                pull(t - 1, subs, (t - 1) % 2, fresh)
            elif before:
                pull(end_tile, before, 1, fresh_before)
            weights(t, subs, t % 2, diag, fresh)

    def all_of(g):
        return [(g, s) for s in range(SUBS)]

    def start(copies):
        for copy in copies:
            copy.start()

    def hops(m):
        return [hop(m, 0), hop(m, 1)]

    start(aux_copies + hops(1))
    visit(all_of(0), None, True, fresh=True)
    start(hops(2))
    visit(all_of(1), all_of(0), True, fresh_before=True)
    start(hops(3))
    for copy in sib_copies + aux_copies:
        copy.wait_recv()
    visit(all_of(2), all_of(1))
    start(hops(4))
    for copy in head:
        copy.wait_recv()
    relay(first).start()
    visit(all_of(first), all_of(first - 1))

    def step(g, carry):
        start(hops(g + 1))
        arrive(g)
        relay(g).start()
        arrive_relay(g)
        visit(all_of(g), all_of(g - 1))
        return carry

    sends_end = last - first - 1
    lax.fori_loop(first + 1, sends_end, step, 0)

    def step_late(g, carry):
        arrive(g)
        relay(g).start()
        arrive_relay(g)
        visit(all_of(g), all_of(g - 1))
        return carry

    lax.fori_loop(sends_end, last - 1, step_late, 0)
    arrive_relay(last - 1)
    rest = [(last, 0), (last, 1), (last - 1, 2), (last - 1, 3)]
    visit(rest, all_of(last - 2))
    arrive(last - 1)
    relay(last - 1).start()
    late = [(last - 1, 0), (last - 1, 1)]
    visit(late, rest)
    arrive_relay(last)
    end = [(last, 2), (last, 3)]
    visit(end, late)
    energy = jnp.zeros((8, LANES), jnp.float32)
    for r in range(0, rows_dev, HOST):
        at = pl.ds(r, HOST)
        energy = energy + jnp.sum((rsum[at, :] * host_s[at, :]).reshape(HOST // 8, 8, LANES), axis=0)
    ebuf[me] = energy
    pull(end_tile, end, 1, False)
    e_copies = [remote(ebuf.at[me], ebuf.at[me], s_e.at[d], e_sem.at[d], (me + d) % ring) for d in range(1, ring)]
    for copy in e_copies:
        copy.start()
    for t in range(hosts):
        at = pl.ds(t * HOST, HOST)
        total = jnp.sum(rsum[at, :], axis=1, keepdims=True)
        sign = host_s[at, :] * (1.0 / feat)
        hx = host_tile(t).astype(jnp.float32)
        f_ref[at, :] = (total * hx - acc[at, :]) * jnp.concatenate([sign, sign], axis=1)

    for copy in head + sib_copies + aux_copies:
        copy.wait_send()

    def drain(g, carry):
        relay(g).wait_send()
        return carry

    lax.fori_loop(first, last, drain, 0)
    def drain_hops(m, carry):
        for copy in hops(m):
            copy.wait_send()
        return carry

    lax.fori_loop(1, sends_end + 1, drain_hops, 0)
    for copy in e_copies:
        copy.wait()
    whole = ebuf[0]
    for d in range(1, ring):
        whole = whole + ebuf[d]
    e_ref[0] = 0.5 * jnp.sum(whole)


def solution(mesh):
    ring = mesh.shape["row"]

    def device_body(pos, chg):
        rows, feat = pos.shape
        groups = ring * rows // (QUANT * SUBS)
        quanta = rows // QUANT
        assert ring == 8 and feat == 2 * LANES and quanta == 8
        dma = pltpu.SemaphoreType.DMA
        f32 = jnp.float32
        vmem = pltpu.VMEM
        scratch = [
            vmem((groups * SUBS, 2, QUANT, LANES), jnp.bfloat16),
            vmem((groups, SUBS, 4, LANES), f32),
            vmem((rows, LANES), f32),
            vmem((rows, LANES), f32),
            vmem((rows, LANES), f32),
            vmem((2, 2 * SUBS, HOST, LANES), jnp.bfloat16),
            vmem((rows, feat), f32),
            vmem((rows, LANES), f32),
            vmem((ring, 8, LANES), f32),
        ]
        for _ in range(2):
            scratch += [dma((2, 2)), dma((groups, 2)), dma((groups,)), dma((3, 2)), dma((15,)), dma((ring,))]
        forces, energy = pl.pallas_call(
            functools.partial(kernel, (groups, rows, ring)),
            out_shape=(jax.ShapeDtypeStruct((rows, feat), f32), jax.ShapeDtypeStruct((1,), f32)),
            in_specs=[pl.BlockSpec(memory_space=pltpu.VMEM), pl.BlockSpec(memory_space=pltpu.VMEM)],
            out_specs=(pl.BlockSpec(memory_space=pltpu.VMEM), pl.BlockSpec(memory_space=pltpu.SMEM)),
            scratch_shapes=scratch,
            compiler_params=pltpu.CompilerParams(collective_id=0, has_side_effects=True, vmem_limit_bytes=40 * 2**20),
            name="pair_forces",
        )(pos.reshape(quanta, QUANT, feat), chg.reshape(rows // LANES, LANES))
        return forces, energy

    return jax.shard_map(device_body, mesh=mesh, in_specs=(P(("sys", "row"), None), P(("sys", "row"))), out_specs=(P(("sys", "row"), None), P("sys")), check_vma=False)
```

```python
import functools
import math

import jax
import jax.numpy as jnp
from jax import lax
from jax.experimental import pallas as pl
from jax.experimental.pallas import tpu as pltpu
from jax.sharding import PartitionSpec as P

LANES = 128
QUANT = 256
SUBS = 4
HOST = 512


def kernel(cfg, x_ref, q_ref, f_ref, e_ref, xs, aux, host_a, host_l, host_s, wts, acc, rsum, ebuf, head_sem, near_sem, relay_sem, sib_sem, aux_sem, e_sem, s_head, s_near, s_relay, s_sib, s_aux, s_e):
    groups, rows_dev, ring = cfg
    feat = x_ref.shape[2]
    log2e = math.log2(math.e)
    dot_scale = 2.0 * log2e / (2.0 * feat)
    sq_scale = -log2e / (2.0 * feat)
    own_groups = rows_dev // (QUANT * SUBS)
    quanta = rows_dev // QUANT
    hosts = rows_dev // HOST
    chunks = rows_dev // LANES
    me = lax.axis_index("row")
    core = me % 2
    sib = me + 1 - 2 * core
    right = (me + 2) % ring
    left = (me + ring - 2) % ring
    right_x = (sib + 2) % ring
    left_x = (sib + ring - 2) % ring
    opp = (me + 4) % ring
    opp_x = (sib + 4) % ring

    def remote(src, dst, send, recv, dev):
        return pltpu.make_async_remote_copy(src_ref=src, dst_ref=dst, send_sem=send, recv_sem=recv, device_id={"row": dev}, device_id_type=pl.DeviceIdType.MESH)

    barrier = pltpu.get_barrier_semaphore()
    for peer in (sib, right, left, right_x, left_x, opp, opp_x):
        pl.semaphore_signal(barrier, inc=1, device_id={"row": peer}, device_id_type=pl.DeviceIdType.MESH)

    first = own_groups + 1
    half = quanta // 2
    far = first + quanta
    last = groups - 1

    def hop(m, turn):
        d = (core + turn) % 2
        on = m // quanta
        src = (1 - on) * ((m + d * half) % quanta) + on * ((first + m - quanta) * SUBS + d)
        dst = (first + m) * SUBS + d
        return remote(xs.at[src], xs.at[dst], s_near.at[m, d], near_sem.at[first + m, d], (me + 2 + d * (ring - 4)) % ring)

    def hop_first(turn):
        d = (core + turn) % 2
        return [remote(x_ref.at[d * half, :, pl.ds(h * LANES, LANES)], xs.at[first * SUBS + d, h], s_head.at[d, h], head_sem.at[d, h], (me + 2 + d * (ring - 4)) % ring) for h in range(2)]

    def relay(g):
        return remote(xs.at[pl.ds(g * SUBS, 2)], xs.at[pl.ds((g + 1) * SUBS + 2, 2)], s_relay.at[g], relay_sem.at[g + 1], sib)

    def arrive(g):
        for d in range(2):
            remote(xs.at[g * SUBS + d], xs.at[g * SUBS + d], s_near.at[0, d], near_sem.at[g, d], me).wait_recv()

    def arrive_relay(g):
        at = pl.ds(g * SUBS + 2, 2)
        remote(xs.at[at], xs.at[at], s_relay.at[0], relay_sem.at[g], me).wait_recv()

    sib_copies = []
    for k, (q, n, at) in enumerate([(0, 4, own_groups * SUBS), (4, 2, first * SUBS + 2), (6, 2, last * SUBS)]):
        for h in range(2):
            sib_copies.append(remote(x_ref.at[pl.ds(q, n), :, pl.ds(h * LANES, LANES)], xs.at[pl.ds(at, n), h], s_sib.at[k, h], sib_sem.at[k, h], sib))
    head = hop_first(0) + hop_first(1)
    pl.semaphore_wait(barrier, 7)
    for copy in head + sib_copies:
        copy.start()
    for g in range(own_groups):
        for s in range(SUBS):
            for h in range(2):
                xs[g * SUBS + s, h] = x_ref[g * SUBS + s, :, h * LANES : (h + 1) * LANES]

    eye = lax.broadcasted_iota(jnp.int32, (LANES, LANES), 0) == lax.broadcasted_iota(jnp.int32, (LANES, LANES), 1)
    for c in range(chunks):
        g, s, r = c // (2 * SUBS), (c // 2) % SUBS, (c % 2) * LANES
        lo = xs[g * SUBS + s, 0, pl.ds(r, LANES), :].astype(jnp.float32)
        hi = xs[g * SUBS + s, 1, pl.ds(r, LANES), :].astype(jnp.float32)
        off = jnp.sum(lo * lo + hi * hi, axis=1, keepdims=True) * sq_scale
        q_row = q_ref[c : c + 1, :]
        aux[g, s, pl.ds(c % 2, 1), :] = jnp.sum(jnp.where(eye, off, 0.0), axis=0, keepdims=True)
        aux[g, s, pl.ds(2 + c % 2, 1), :] = q_row
        q_col = jnp.sum(jnp.where(eye, q_row, 0.0), axis=1, keepdims=True)
        mag = jnp.log(jnp.abs(q_col)) * log2e
        wide = (LANES, LANES)
        host_a[pl.ds(c * LANES, LANES), :] = jnp.broadcast_to(off + mag, wide)
        host_l[pl.ds(c * LANES, LANES), :] = jnp.broadcast_to(mag, wide)
        host_s[pl.ds(c * LANES, LANES), :] = jnp.broadcast_to(jnp.where(q_col < 0.0, -1.0, 1.0), wide)

    aux_plan = [
        (aux.at[0], aux.at[own_groups], sib),
        (aux.at[1, pl.ds(0, 2)], aux.at[first, pl.ds(2, 2)], sib),
        (aux.at[1, pl.ds(2, 2)], aux.at[last, pl.ds(0, 2)], sib),
    ]
    for h in range(2):
        at, turned = first + half * h, first + half * (1 - h)
        aux_plan += [
            (aux.at[h], aux.at[pl.ds(at, half), 0], right),
            (aux.at[h], aux.at[pl.ds(turned, half), 1], left),
            (aux.at[h], aux.at[pl.ds(at + 1, half), 2], right_x),
            (aux.at[h], aux.at[pl.ds(turned + 1, half), 3], left_x),
            (aux.at[h], aux.at[pl.ds(far, half), h], opp),
            (aux.at[h], aux.at[pl.ds(far + 1, half), 2 + h], opp_x),
        ]
    aux_copies = [remote(src, dst, s_aux.at[n], aux_sem.at[n], dev) for n, (src, dst, dev) in enumerate(aux_plan)]
    def tile(g, s):
        return jnp.concatenate([xs[g * SUBS + s, 0], xs[g * SUBS + s, 1]], axis=1)

    def host_tile(t):
        return jnp.concatenate([tile(t * 2 // SUBS, t * 2 % SUBS), tile((t * 2 + 1) // SUBS, (t * 2 + 1) % SUBS)], axis=0)

    def dots(t, g, s):
        return lax.dot_general(host_tile(t), tile(g, s), (((1,), (1,)), ((), ())), preferred_element_type=jnp.float32)

    def emit(prod, t, n, g, s, slot, diag, fresh):
        base = t * HOST
        step = LANES if diag else HOST
        for r in range(0, HOST, step):
            at = pl.ds(base + r, step)
            off, cap = host_a[at, :], host_l[at, :]
            total = None if fresh else rsum[at, :]
            for c in range(2):
                power = prod(r, step, c) * dot_scale + off + aux[g, s, pl.ds(c, 1), :]
                w = jnp.exp2(jnp.minimum(power, cap)) * aux[g, s, pl.ds(2 + c, 1), :]
                if diag and base + r == (g * SUBS + s) * QUANT + c * LANES:
                    w = jnp.where(eye, 0.0, w)
                total = w if total is None else total + w
                wts[slot, 2 * n + c, pl.ds(r, step), :] = w.astype(jnp.bfloat16)
            rsum[at, :] = total

    def weights(t, subs, slot, diag, fresh):
        for n, (g, s) in enumerate(subs):
            p = dots(t, g, s)
            emit(lambda r, step, c: p[r : r + step, c * LANES : (c + 1) * LANES], t, n, g, s, slot, diag, fresh and n == 0)

    def pull(t, subs, slot, fresh):
        part = None
        for n, (g, s) in enumerate(subs):
            w = jnp.concatenate([wts[slot, 2 * n], wts[slot, 2 * n + 1]], axis=1)
            d = jnp.dot(w, tile(g, s), preferred_element_type=jnp.float32)
            part = d if part is None else part + d
        at = pl.ds(t * HOST, HOST)
        acc[at, :] = part if fresh else acc[at, :] + part

    end_tile = hosts - 1

    def visit(subs, before, diag=False, fresh=False, fresh_before=False):
        for t in range(hosts):
            if t > 0:
                pull(t - 1, subs, (t - 1) % 2, fresh)
            elif before:
                pull(end_tile, before, 1, fresh_before)
            weights(t, subs, t % 2, diag, fresh)

    def all_of(g):
        return [(g, s) for s in range(SUBS)]

    def start(copies):
        for copy in copies:
            copy.start()

    def hops(m):
        return [hop(m, 0), hop(m, 1)]

    start(aux_copies + hops(1) + hops(2))
    visit(all_of(0), None, True, fresh=True)
    start(hops(3))
    visit(all_of(1), all_of(0), True, fresh_before=True)
    start(hops(4) + hops(5))
    for copy in sib_copies + aux_copies:
        copy.wait_recv()
    visit(all_of(2), all_of(1))
    start(hops(6))
    for copy in head:
        copy.wait_recv()
    relay(first).start()
    visit(all_of(first), all_of(first - 1))

    def step(g, carry):
        start(hops(g + 3))
        arrive(g)
        relay(g).start()
        arrive_relay(g)
        visit(all_of(g), all_of(g - 1))
        return carry

    sends_end = last - first - 3
    lax.fori_loop(first + 1, sends_end, step, 0)

    def step_late(g, carry):
        arrive(g)
        relay(g).start()
        arrive_relay(g)
        visit(all_of(g), all_of(g - 1))
        return carry

    lax.fori_loop(sends_end, last - 1, step_late, 0)
    arrive_relay(last - 1)
    rest = [(last, 0), (last, 1), (last - 1, 2), (last - 1, 3)]
    visit(rest, all_of(last - 2))
    arrive(last - 1)
    relay(last - 1).start()
    late = [(last - 1, 0), (last - 1, 1)]
    visit(late, rest)
    arrive_relay(last)
    end = [(last, 2), (last, 3)]
    visit(end, late)
    energy = jnp.zeros((8, LANES), jnp.float32)
    for r in range(0, rows_dev, HOST):
        at = pl.ds(r, HOST)
        energy = energy + jnp.sum((rsum[at, :] * host_s[at, :]).reshape(HOST // 8, 8, LANES), axis=0)
    ebuf[me] = energy
    pull(end_tile, end, 1, False)
    e_copies = [remote(ebuf.at[me], ebuf.at[me], s_e.at[d], e_sem.at[d], (me + d) % ring) for d in range(1, ring)]
    for copy in e_copies:
        copy.start()
    for t in range(hosts):
        at = pl.ds(t * HOST, HOST)
        total = jnp.sum(rsum[at, :], axis=1, keepdims=True)
        sign = host_s[at, :] * (1.0 / feat)
        hx = host_tile(t).astype(jnp.float32)
        f_ref[at, :] = (total * hx - acc[at, :]) * jnp.concatenate([sign, sign], axis=1)

    for copy in head + sib_copies + aux_copies:
        copy.wait_send()

    def drain(g, carry):
        relay(g).wait_send()
        return carry

    lax.fori_loop(first, last, drain, 0)
    def drain_hops(m, carry):
        for copy in hops(m):
            copy.wait_send()
        return carry

    lax.fori_loop(1, sends_end + 3, drain_hops, 0)
    for copy in e_copies:
        copy.wait()
    whole = ebuf[0]
    for d in range(1, ring):
        whole = whole + ebuf[d]
    e_ref[0] = 0.5 * jnp.sum(whole)


def solution(mesh):
    ring = mesh.shape["row"]

    def device_body(pos, chg):
        rows, feat = pos.shape
        groups = ring * rows // (QUANT * SUBS)
        quanta = rows // QUANT
        assert ring == 8 and feat == 2 * LANES and quanta == 8
        dma = pltpu.SemaphoreType.DMA
        f32 = jnp.float32
        vmem = pltpu.VMEM
        scratch = [
            vmem((groups * SUBS, 2, QUANT, LANES), jnp.bfloat16),
            vmem((groups, SUBS, 4, LANES), f32),
            vmem((rows, LANES), f32),
            vmem((rows, LANES), f32),
            vmem((rows, LANES), f32),
            vmem((2, 2 * SUBS, HOST, LANES), jnp.bfloat16),
            vmem((rows, feat), f32),
            vmem((rows, LANES), f32),
            vmem((ring, 8, LANES), f32),
        ]
        for _ in range(2):
            scratch += [dma((2, 2)), dma((groups, 2)), dma((groups,)), dma((3, 2)), dma((15,)), dma((ring,))]
        forces, energy = pl.pallas_call(
            functools.partial(kernel, (groups, rows, ring)),
            out_shape=(jax.ShapeDtypeStruct((rows, feat), f32), jax.ShapeDtypeStruct((1,), f32)),
            in_specs=[pl.BlockSpec(memory_space=pltpu.VMEM), pl.BlockSpec(memory_space=pltpu.VMEM)],
            out_specs=(pl.BlockSpec(memory_space=pltpu.VMEM), pl.BlockSpec(memory_space=pltpu.SMEM)),
            scratch_shapes=scratch,
            compiler_params=pltpu.CompilerParams(collective_id=0, has_side_effects=True, vmem_limit_bytes=40 * 2**20),
            name="pair_forces",
        )(pos.reshape(quanta, QUANT, feat), chg.reshape(rows // LANES, LANES))
        return forces, energy

    return jax.shard_map(device_body, mesh=mesh, in_specs=(P(("sys", "row"), None), P(("sys", "row"))), out_specs=(P(("sys", "row"), None), P("sys")), check_vma=False)
```

```python
import functools
import math

import jax
import jax.numpy as jnp
from jax import lax
from jax.experimental import pallas as pl
from jax.experimental.pallas import tpu as pltpu
from jax.sharding import PartitionSpec as P

LANES = 128
QUANT = 256
SUBS = 4
HOST = 512


def kernel(cfg, x_ref, q_ref, f_ref, e_ref, xs, aux, host_a, host_l, host_s, wts, acc, rsum, ebuf, head_sem, near_sem, relay_sem, sib_sem, aux_sem, e_sem, s_head, s_near, s_relay, s_sib, s_aux, s_e):
    groups, rows_dev, ring = cfg
    feat = x_ref.shape[2]
    log2e = math.log2(math.e)
    dot_scale = 2.0 * log2e / (2.0 * feat)
    sq_scale = -log2e / (2.0 * feat)
    own_groups = rows_dev // (QUANT * SUBS)
    quanta = rows_dev // QUANT
    hosts = rows_dev // HOST
    chunks = rows_dev // LANES
    me = lax.axis_index("row")
    core = me % 2
    sib = me + 1 - 2 * core
    right = (me + 2) % ring
    left = (me + ring - 2) % ring
    right_x = (sib + 2) % ring
    left_x = (sib + ring - 2) % ring
    opp = (me + 4) % ring
    opp_x = (sib + 4) % ring

    def remote(src, dst, send, recv, dev):
        return pltpu.make_async_remote_copy(src_ref=src, dst_ref=dst, send_sem=send, recv_sem=recv, device_id={"row": dev}, device_id_type=pl.DeviceIdType.MESH)

    barrier = pltpu.get_barrier_semaphore()
    for peer in (sib, right, left, right_x, left_x, opp, opp_x):
        pl.semaphore_signal(barrier, inc=1, device_id={"row": peer}, device_id_type=pl.DeviceIdType.MESH)

    first = own_groups + 1
    half = quanta // 2
    far = first + quanta
    last = groups - 1

    def hop(m, turn):
        d = (core + turn) % 2
        on = m // quanta
        src = (1 - on) * ((m + d * half) % quanta) + on * ((first + m - quanta) * SUBS + d)
        dst = (first + m) * SUBS + d
        return remote(xs.at[src], xs.at[dst], s_near.at[m, d], near_sem.at[first + m, d], (me + 2 + d * (ring - 4)) % ring)

    def hop_first(turn):
        d = (core + turn) % 2
        return [remote(x_ref.at[d * half, :, pl.ds(h * LANES, LANES)], xs.at[first * SUBS + d, h], s_head.at[d, h], head_sem.at[d, h], (me + 2 + d * (ring - 4)) % ring) for h in range(2)]

    def relay(g):
        return remote(xs.at[pl.ds(g * SUBS, 2)], xs.at[pl.ds((g + 1) * SUBS + 2, 2)], s_relay.at[g], relay_sem.at[g + 1], sib)

    def arrive(g):
        for d in range(2):
            remote(xs.at[g * SUBS + d], xs.at[g * SUBS + d], s_near.at[0, d], near_sem.at[g, d], me).wait_recv()

    def arrive_relay(g):
        at = pl.ds(g * SUBS + 2, 2)
        remote(xs.at[at], xs.at[at], s_relay.at[0], relay_sem.at[g], me).wait_recv()

    sib_copies = []
    for k, (q, n, at) in enumerate([(0, 4, own_groups * SUBS), (4, 2, first * SUBS + 2), (6, 2, last * SUBS)]):
        for h in range(2):
            sib_copies.append(remote(x_ref.at[pl.ds(q, n), :, pl.ds(h * LANES, LANES)], xs.at[pl.ds(at, n), h], s_sib.at[k, h], sib_sem.at[k, h], sib))
    head = hop_first(0) + hop_first(1)
    for g in range(own_groups):
        for s in range(SUBS):
            for h in range(2):
                xs[g * SUBS + s, h] = x_ref[g * SUBS + s, :, h * LANES : (h + 1) * LANES]

    eye = lax.broadcasted_iota(jnp.int32, (LANES, LANES), 0) == lax.broadcasted_iota(jnp.int32, (LANES, LANES), 1)
    for c in range(chunks):
        g, s, r = c // (2 * SUBS), (c // 2) % SUBS, (c % 2) * LANES
        lo = xs[g * SUBS + s, 0, pl.ds(r, LANES), :].astype(jnp.float32)
        hi = xs[g * SUBS + s, 1, pl.ds(r, LANES), :].astype(jnp.float32)
        off = jnp.sum(lo * lo + hi * hi, axis=1, keepdims=True) * sq_scale
        q_row = q_ref[c : c + 1, :]
        aux[g, s, pl.ds(c % 2, 1), :] = jnp.sum(jnp.where(eye, off, 0.0), axis=0, keepdims=True)
        aux[g, s, pl.ds(2 + c % 2, 1), :] = q_row
        q_col = jnp.sum(jnp.where(eye, q_row, 0.0), axis=1, keepdims=True)
        mag = jnp.log(jnp.abs(q_col)) * log2e
        wide = (LANES, LANES)
        host_a[pl.ds(c * LANES, LANES), :] = jnp.broadcast_to(off + mag, wide)
        host_l[pl.ds(c * LANES, LANES), :] = jnp.broadcast_to(mag, wide)
        host_s[pl.ds(c * LANES, LANES), :] = jnp.broadcast_to(jnp.where(q_col < 0.0, -1.0, 1.0), wide)

    pl.semaphore_wait(barrier, 7)
    for copy in head + sib_copies:
        copy.start()

    aux_plan = [
        (aux.at[0], aux.at[own_groups], sib),
        (aux.at[1, pl.ds(0, 2)], aux.at[first, pl.ds(2, 2)], sib),
        (aux.at[1, pl.ds(2, 2)], aux.at[last, pl.ds(0, 2)], sib),
    ]
    for h in range(2):
        at, turned = first + half * h, first + half * (1 - h)
        aux_plan += [
            (aux.at[h], aux.at[pl.ds(at, half), 0], right),
            (aux.at[h], aux.at[pl.ds(turned, half), 1], left),
            (aux.at[h], aux.at[pl.ds(at + 1, half), 2], right_x),
            (aux.at[h], aux.at[pl.ds(turned + 1, half), 3], left_x),
            (aux.at[h], aux.at[pl.ds(far, half), h], opp),
            (aux.at[h], aux.at[pl.ds(far + 1, half), 2 + h], opp_x),
        ]
    aux_copies = [remote(src, dst, s_aux.at[n], aux_sem.at[n], dev) for n, (src, dst, dev) in enumerate(aux_plan)]
    def tile(g, s):
        return jnp.concatenate([xs[g * SUBS + s, 0], xs[g * SUBS + s, 1]], axis=1)

    def host_tile(t):
        return jnp.concatenate([tile(t * 2 // SUBS, t * 2 % SUBS), tile((t * 2 + 1) // SUBS, (t * 2 + 1) % SUBS)], axis=0)

    def dots(t, g, s):
        return lax.dot_general(host_tile(t), tile(g, s), (((1,), (1,)), ((), ())), preferred_element_type=jnp.float32)

    def emit(prod, t, n, g, s, slot, diag, fresh):
        base = t * HOST
        step = LANES if diag else HOST
        for r in range(0, HOST, step):
            at = pl.ds(base + r, step)
            off, cap = host_a[at, :], host_l[at, :]
            total = None if fresh else rsum[at, :]
            for c in range(2):
                power = prod(r, step, c) * dot_scale + off + aux[g, s, pl.ds(c, 1), :]
                w = jnp.exp2(jnp.minimum(power, cap)) * aux[g, s, pl.ds(2 + c, 1), :]
                if diag and base + r == (g * SUBS + s) * QUANT + c * LANES:
                    w = jnp.where(eye, 0.0, w)
                total = w if total is None else total + w
                wts[slot, 2 * n + c, pl.ds(r, step), :] = w.astype(jnp.bfloat16)
            rsum[at, :] = total

    def weights(t, subs, slot, diag, fresh):
        for n, (g, s) in enumerate(subs):
            p = dots(t, g, s)
            emit(lambda r, step, c: p[r : r + step, c * LANES : (c + 1) * LANES], t, n, g, s, slot, diag, fresh and n == 0)

    def pull(t, subs, slot, fresh):
        part = None
        for n, (g, s) in enumerate(subs):
            w = jnp.concatenate([wts[slot, 2 * n], wts[slot, 2 * n + 1]], axis=1)
            d = jnp.dot(w, tile(g, s), preferred_element_type=jnp.float32)
            part = d if part is None else part + d
        at = pl.ds(t * HOST, HOST)
        acc[at, :] = part if fresh else acc[at, :] + part

    end_tile = hosts - 1

    def visit(subs, before, diag=False, fresh=False, fresh_before=False):
        for t in range(hosts):
            if t > 0:
                pull(t - 1, subs, (t - 1) % 2, fresh)
            elif before:
                pull(end_tile, before, 1, fresh_before)
            weights(t, subs, t % 2, diag, fresh)

    def all_of(g):
        return [(g, s) for s in range(SUBS)]

    def start(copies):
        for copy in copies:
            copy.start()

    def hops(m):
        return [hop(m, 0), hop(m, 1)]

    start(aux_copies + hops(1) + hops(2))
    visit(all_of(0), None, True, fresh=True)
    start(hops(3))
    visit(all_of(1), all_of(0), True, fresh_before=True)
    start(hops(4) + hops(5))
    for copy in sib_copies + aux_copies:
        copy.wait_recv()
    visit(all_of(2), all_of(1))
    start(hops(6))
    for copy in head:
        copy.wait_recv()
    relay(first).start()
    visit(all_of(first), all_of(first - 1))

    def step(g, carry):
        start(hops(g + 3))
        arrive(g)
        relay(g).start()
        arrive_relay(g)
        visit(all_of(g), all_of(g - 1))
        return carry

    sends_end = last - first - 3
    lax.fori_loop(first + 1, sends_end, step, 0)

    def step_late(g, carry):
        arrive(g)
        relay(g).start()
        arrive_relay(g)
        visit(all_of(g), all_of(g - 1))
        return carry

    lax.fori_loop(sends_end, last - 1, step_late, 0)
    arrive_relay(last - 1)
    rest = [(last, 0), (last, 1), (last - 1, 2), (last - 1, 3)]
    visit(rest, all_of(last - 2))
    arrive(last - 1)
    relay(last - 1).start()
    late = [(last - 1, 0), (last - 1, 1)]
    visit(late, rest)
    arrive_relay(last)
    end = [(last, 2), (last, 3)]
    visit(end, late)
    energy = jnp.zeros((8, LANES), jnp.float32)
    for r in range(0, rows_dev, HOST):
        at = pl.ds(r, HOST)
        energy = energy + jnp.sum((rsum[at, :] * host_s[at, :]).reshape(HOST // 8, 8, LANES), axis=0)
    ebuf[me] = energy
    def result(t):
        at = pl.ds(t * HOST, HOST)
        total = jnp.sum(rsum[at, :], axis=1, keepdims=True)
        sign = host_s[at, :] * (1.0 / feat)
        hx = host_tile(t).astype(jnp.float32)
        f_ref[at, :] = (total * hx - acc[at, :]) * jnp.concatenate([sign, sign], axis=1)

    result(0)
    e_copies = [remote(ebuf.at[me], ebuf.at[me], s_e.at[d], e_sem.at[d], (me + d) % ring) for d in range(1, ring)]
    for copy in e_copies:
        copy.start()
    pull(end_tile, end, 1, False)
    for t in range(1, hosts):
        result(t)

    for copy in head + sib_copies + aux_copies:
        copy.wait_send()

    def drain(g, carry):
        relay(g).wait_send()
        return carry

    lax.fori_loop(first, last, drain, 0)
    def drain_hops(m, carry):
        for copy in hops(m):
            copy.wait_send()
        return carry

    lax.fori_loop(1, sends_end + 3, drain_hops, 0)
    for copy in e_copies:
        copy.wait()
    whole = ebuf[0]
    for d in range(1, ring):
        whole = whole + ebuf[d]
    e_ref[0] = 0.5 * jnp.sum(whole)


def solution(mesh):
    ring = mesh.shape["row"]

    def device_body(pos, chg):
        rows, feat = pos.shape
        groups = ring * rows // (QUANT * SUBS)
        quanta = rows // QUANT
        assert ring == 8 and feat == 2 * LANES and quanta == 8
        dma = pltpu.SemaphoreType.DMA
        f32 = jnp.float32
        vmem = pltpu.VMEM
        scratch = [
            vmem((groups * SUBS, 2, QUANT, LANES), jnp.bfloat16),
            vmem((groups, SUBS, 4, LANES), f32),
            vmem((rows, LANES), f32),
            vmem((rows, LANES), f32),
            vmem((rows, LANES), f32),
            vmem((2, 2 * SUBS, HOST, LANES), jnp.bfloat16),
            vmem((rows, feat), f32),
            vmem((rows, LANES), f32),
            vmem((ring, 8, LANES), f32),
        ]
        for _ in range(2):
            scratch += [dma((2, 2)), dma((groups, 2)), dma((groups,)), dma((3, 2)), dma((15,)), dma((ring,))]
        forces, energy = pl.pallas_call(
            functools.partial(kernel, (groups, rows, ring)),
            out_shape=(jax.ShapeDtypeStruct((rows, feat), f32), jax.ShapeDtypeStruct((1,), f32)),
            in_specs=[pl.BlockSpec(memory_space=pltpu.VMEM), pl.BlockSpec(memory_space=pltpu.VMEM)],
            out_specs=(pl.BlockSpec(memory_space=pltpu.VMEM), pl.BlockSpec(memory_space=pltpu.SMEM)),
            scratch_shapes=scratch,
            compiler_params=pltpu.CompilerParams(collective_id=0, has_side_effects=True, vmem_limit_bytes=40 * 2**20),
            name="pair_forces",
        )(pos.reshape(quanta, QUANT, feat), chg.reshape(rows // LANES, LANES))
        return forces, energy

    return jax.shard_map(device_body, mesh=mesh, in_specs=(P(("sys", "row"), None), P(("sys", "row"))), out_specs=(P(("sys", "row"), None), P("sys")), check_vma=False)
```

```python
import functools
import math

import jax
import jax.numpy as jnp
from jax import lax
from jax.experimental import pallas as pl
from jax.experimental.pallas import tpu as pltpu
from jax.sharding import PartitionSpec as P

LANES = 128
QUANT = 256
SUBS = 4
HOST = 512


def kernel(cfg, x_ref, q_ref, f_ref, e_ref, xs, aux, host_a, host_l, host_s, wts, acc, rsum, ebuf, head_sem, near_sem, relay_sem, sib_sem, aux_sem, e_sem, s_head, s_near, s_relay, s_sib, s_aux, s_e, s_cross):
    groups, rows_dev, ring = cfg
    feat = x_ref.shape[2]
    log2e = math.log2(math.e)
    dot_scale = 2.0 * log2e / (2.0 * feat)
    sq_scale = -log2e / (2.0 * feat)
    own_groups = rows_dev // (QUANT * SUBS)
    quanta = rows_dev // QUANT
    hosts = rows_dev // HOST
    chunks = rows_dev // LANES
    me = lax.axis_index("row")
    core = me % 2
    sib = me + 1 - 2 * core
    right = (me + 2) % ring
    left = (me + ring - 2) % ring
    right_x = (sib + 2) % ring
    left_x = (sib + ring - 2) % ring
    opp = (me + 4) % ring
    opp_x = (sib + 4) % ring

    def remote(src, dst, send, recv, dev):
        return pltpu.make_async_remote_copy(src_ref=src, dst_ref=dst, send_sem=send, recv_sem=recv, device_id={"row": dev}, device_id_type=pl.DeviceIdType.MESH)

    barrier = pltpu.get_barrier_semaphore()
    for peer in (sib, right, left, right_x, left_x, opp, opp_x):
        pl.semaphore_signal(barrier, inc=1, device_id={"row": peer}, device_id_type=pl.DeviceIdType.MESH)

    first = own_groups + 1
    half = quanta // 2
    far = first + quanta
    last = groups - 1

    def hop(m, turn):
        d = (core + turn) % 2
        on = m // quanta
        src = (1 - on) * ((m + d * half) % quanta) + on * ((first + m - quanta) * SUBS + d)
        dst = (first + m) * SUBS + d
        return remote(xs.at[src], xs.at[dst], s_near.at[m, d], near_sem.at[first + m, d], (me + 2 + d * (ring - 4)) % ring)

    def cross(m, d):
        src = (first + m - quanta + 1) * SUBS + 2 + d
        dst = (first + m) * SUBS + d
        return remote(xs.at[src], xs.at[dst], s_cross.at[m, d], near_sem.at[first + m, d], (sib + 2 + d * (ring - 4)) % ring)

    def hop_first(turn):
        d = (core + turn) % 2
        return [remote(x_ref.at[d * half, :, pl.ds(h * LANES, LANES)], xs.at[first * SUBS + d, h], s_head.at[d, h], head_sem.at[d, h], (me + 2 + d * (ring - 4)) % ring) for h in range(2)]

    def relay(g):
        return remote(xs.at[pl.ds(g * SUBS, 2)], xs.at[pl.ds((g + 1) * SUBS + 2, 2)], s_relay.at[g], relay_sem.at[g + 1], sib)

    def arrive(g):
        for d in range(2):
            remote(xs.at[g * SUBS + d], xs.at[g * SUBS + d], s_near.at[0, d], near_sem.at[g, d], me).wait_recv()

    def arrive_relay(g):
        at = pl.ds(g * SUBS + 2, 2)
        remote(xs.at[at], xs.at[at], s_relay.at[0], relay_sem.at[g], me).wait_recv()

    sib_copies = []
    for k, (q, n, at) in enumerate([(0, 4, own_groups * SUBS), (4, 2, first * SUBS + 2), (6, 2, last * SUBS)]):
        for h in range(2):
            sib_copies.append(remote(x_ref.at[pl.ds(q, n), :, pl.ds(h * LANES, LANES)], xs.at[pl.ds(at, n), h], s_sib.at[k, h], sib_sem.at[k, h], sib))
    head = hop_first(0) + hop_first(1)
    for g in range(own_groups):
        for s in range(SUBS):
            for h in range(2):
                xs[g * SUBS + s, h] = x_ref[g * SUBS + s, :, h * LANES : (h + 1) * LANES]

    eye = lax.broadcasted_iota(jnp.int32, (LANES, LANES), 0) == lax.broadcasted_iota(jnp.int32, (LANES, LANES), 1)
    for c in range(chunks):
        g, s, r = c // (2 * SUBS), (c // 2) % SUBS, (c % 2) * LANES
        lo = xs[g * SUBS + s, 0, pl.ds(r, LANES), :].astype(jnp.float32)
        hi = xs[g * SUBS + s, 1, pl.ds(r, LANES), :].astype(jnp.float32)
        off = jnp.sum(lo * lo + hi * hi, axis=1, keepdims=True) * sq_scale
        q_row = q_ref[c : c + 1, :]
        aux[g, s, pl.ds(c % 2, 1), :] = jnp.sum(jnp.where(eye, off, 0.0), axis=0, keepdims=True)
        aux[g, s, pl.ds(2 + c % 2, 1), :] = q_row
        q_col = jnp.sum(jnp.where(eye, q_row, 0.0), axis=1, keepdims=True)
        mag = jnp.log(jnp.abs(q_col)) * log2e
        wide = (LANES, LANES)
        host_a[pl.ds(c * LANES, LANES), :] = jnp.broadcast_to(off + mag, wide)
        host_l[pl.ds(c * LANES, LANES), :] = jnp.broadcast_to(mag, wide)
        host_s[pl.ds(c * LANES, LANES), :] = jnp.broadcast_to(jnp.where(q_col < 0.0, -1.0, 1.0), wide)

    pl.semaphore_wait(barrier, 7)
    for copy in head + sib_copies:
        copy.start()

    aux_plan = [
        (aux.at[0], aux.at[own_groups], sib),
        (aux.at[1, pl.ds(0, 2)], aux.at[first, pl.ds(2, 2)], sib),
        (aux.at[1, pl.ds(2, 2)], aux.at[last, pl.ds(0, 2)], sib),
    ]
    for h in range(2):
        at, turned = first + half * h, first + half * (1 - h)
        aux_plan += [
            (aux.at[h], aux.at[pl.ds(at, half), 0], right),
            (aux.at[h], aux.at[pl.ds(turned, half), 1], left),
            (aux.at[h], aux.at[pl.ds(at + 1, half), 2], right_x),
            (aux.at[h], aux.at[pl.ds(turned + 1, half), 3], left_x),
            (aux.at[h], aux.at[pl.ds(far, half), h], opp),
            (aux.at[h], aux.at[pl.ds(far + 1, half), 2 + h], opp_x),
        ]
    aux_copies = [remote(src, dst, s_aux.at[n], aux_sem.at[n], dev) for n, (src, dst, dev) in enumerate(aux_plan)]
    def tile(g, s):
        return jnp.concatenate([xs[g * SUBS + s, 0], xs[g * SUBS + s, 1]], axis=1)

    def host_tile(t):
        return jnp.concatenate([tile(t * 2 // SUBS, t * 2 % SUBS), tile((t * 2 + 1) // SUBS, (t * 2 + 1) % SUBS)], axis=0)

    def dots(t, g, s):
        return lax.dot_general(host_tile(t), tile(g, s), (((1,), (1,)), ((), ())), preferred_element_type=jnp.float32)

    def emit(prod, t, n, g, s, slot, diag, fresh):
        base = t * HOST
        step = LANES if diag else HOST
        for r in range(0, HOST, step):
            at = pl.ds(base + r, step)
            off, cap = host_a[at, :], host_l[at, :]
            total = None if fresh else rsum[at, :]
            for c in range(2):
                power = prod(r, step, c) * dot_scale + off + aux[g, s, pl.ds(c, 1), :]
                w = jnp.exp2(jnp.minimum(power, cap)) * aux[g, s, pl.ds(2 + c, 1), :]
                if diag and base + r == (g * SUBS + s) * QUANT + c * LANES:
                    w = jnp.where(eye, 0.0, w)
                total = w if total is None else total + w
                wts[slot, 2 * n + c, pl.ds(r, step), :] = w.astype(jnp.bfloat16)
            rsum[at, :] = total

    def weights(t, subs, slot, diag, fresh):
        for n, (g, s) in enumerate(subs):
            p = dots(t, g, s)
            emit(lambda r, step, c: p[r : r + step, c * LANES : (c + 1) * LANES], t, n, g, s, slot, diag, fresh and n == 0)

    def pull(t, subs, slot, fresh):
        part = None
        for n, (g, s) in enumerate(subs):
            w = jnp.concatenate([wts[slot, 2 * n], wts[slot, 2 * n + 1]], axis=1)
            d = jnp.dot(w, tile(g, s), preferred_element_type=jnp.float32)
            part = d if part is None else part + d
        at = pl.ds(t * HOST, HOST)
        acc[at, :] = part if fresh else acc[at, :] + part

    end_tile = hosts - 1

    def visit(subs, before, diag=False, fresh=False, fresh_before=False):
        for t in range(hosts):
            if t > 0:
                pull(t - 1, subs, (t - 1) % 2, fresh)
            elif before:
                pull(end_tile, before, 1, fresh_before)
            weights(t, subs, t % 2, diag, fresh)

    def all_of(g):
        return [(g, s) for s in range(SUBS)]

    def start(copies):
        for copy in copies:
            copy.start()

    def hops(m):
        return [hop(m, 0), hop(m, 1)]

    start(aux_copies + hops(1) + hops(2))
    visit(all_of(0), None, True, fresh=True)
    start(hops(3))
    visit(all_of(1), all_of(0), True, fresh_before=True)
    start(hops(4) + hops(5))
    for copy in sib_copies + aux_copies:
        copy.wait_recv()
    visit(all_of(2), all_of(1))
    start(hops(6))
    for copy in head:
        copy.wait_recv()
    relay(first).start()
    visit(all_of(first), all_of(first - 1))

    def step(g, carry):
        m = g + 3

        @pl.when(m < quanta)
        def _():
            start(hops(m))

        @pl.when((m >= quanta) & (core == 1))
        def _():
            start(hops(m) + [cross(m, 0), cross(m, 1)])

        arrive(g)
        relay(g).start()
        arrive_relay(g)
        visit(all_of(g), all_of(g - 1))
        return carry

    sends_end = last - first - 3
    lax.fori_loop(first + 1, sends_end, step, 0)

    def step_late(g, carry):
        arrive(g)
        relay(g).start()
        arrive_relay(g)
        visit(all_of(g), all_of(g - 1))
        return carry

    lax.fori_loop(sends_end, last - 1, step_late, 0)
    arrive_relay(last - 1)
    rest = [(last, 0), (last, 1), (last - 1, 2), (last - 1, 3)]
    visit(rest, all_of(last - 2))
    arrive(last - 1)
    relay(last - 1).start()
    late = [(last - 1, 0), (last - 1, 1)]
    visit(late, rest)
    arrive_relay(last)
    end = [(last, 2), (last, 3)]
    visit(end, late)
    energy = jnp.zeros((8, LANES), jnp.float32)
    for r in range(0, rows_dev, HOST):
        at = pl.ds(r, HOST)
        energy = energy + jnp.sum((rsum[at, :] * host_s[at, :]).reshape(HOST // 8, 8, LANES), axis=0)
    ebuf[me] = energy
    def result(t):
        at = pl.ds(t * HOST, HOST)
        total = jnp.sum(rsum[at, :], axis=1, keepdims=True)
        sign = host_s[at, :] * (1.0 / feat)
        hx = host_tile(t).astype(jnp.float32)
        f_ref[at, :] = (total * hx - acc[at, :]) * jnp.concatenate([sign, sign], axis=1)

    result(0)
    e_copies = [remote(ebuf.at[me], ebuf.at[me], s_e.at[d], e_sem.at[d], (me + d) % ring) for d in range(1, ring)]
    for copy in e_copies:
        copy.start()
    pull(end_tile, end, 1, False)
    for t in range(1, hosts):
        result(t)

    for copy in head + sib_copies + aux_copies:
        copy.wait_send()

    def drain(g, carry):
        relay(g).wait_send()
        return carry

    lax.fori_loop(first, last, drain, 0)
    def drain_hops(m, carry):
        for copy in hops(m):
            copy.wait_send()
        return carry

    lax.fori_loop(1, quanta, drain_hops, 0)

    @pl.when(core == 1)
    def _():
        for m in range(quanta, sends_end + 3):
            for copy in hops(m) + [cross(m, 0), cross(m, 1)]:
                copy.wait_send()

    for copy in e_copies:
        copy.wait()
    whole = ebuf[0]
    for d in range(1, ring):
        whole = whole + ebuf[d]
    e_ref[0] = 0.5 * jnp.sum(whole)


def solution(mesh):
    ring = mesh.shape["row"]

    def device_body(pos, chg):
        rows, feat = pos.shape
        groups = ring * rows // (QUANT * SUBS)
        quanta = rows // QUANT
        assert ring == 8 and feat == 2 * LANES and quanta == 8
        dma = pltpu.SemaphoreType.DMA
        f32 = jnp.float32
        vmem = pltpu.VMEM
        scratch = [
            vmem((groups * SUBS, 2, QUANT, LANES), jnp.bfloat16),
            vmem((groups, SUBS, 4, LANES), f32),
            vmem((rows, LANES), f32),
            vmem((rows, LANES), f32),
            vmem((rows, LANES), f32),
            vmem((2, 2 * SUBS, HOST, LANES), jnp.bfloat16),
            vmem((rows, feat), f32),
            vmem((rows, LANES), f32),
            vmem((ring, 8, LANES), f32),
        ]
        for _ in range(2):
            scratch += [dma((2, 2)), dma((groups, 2)), dma((groups,)), dma((3, 2)), dma((15,)), dma((ring,))]
        scratch.append(dma((groups, 2)))
        forces, energy = pl.pallas_call(
            functools.partial(kernel, (groups, rows, ring)),
            out_shape=(jax.ShapeDtypeStruct((rows, feat), f32), jax.ShapeDtypeStruct((1,), f32)),
            in_specs=[pl.BlockSpec(memory_space=pltpu.VMEM), pl.BlockSpec(memory_space=pltpu.VMEM)],
            out_specs=(pl.BlockSpec(memory_space=pltpu.VMEM), pl.BlockSpec(memory_space=pltpu.SMEM)),
            scratch_shapes=scratch,
            compiler_params=pltpu.CompilerParams(collective_id=0, has_side_effects=True, vmem_limit_bytes=40 * 2**20),
            name="pair_forces",
        )(pos.reshape(quanta, QUANT, feat), chg.reshape(rows // LANES, LANES))
        return forces, energy

    return jax.shard_map(device_body, mesh=mesh, in_specs=(P(("sys", "row"), None), P(("sys", "row"))), out_specs=(P(("sys", "row"), None), P("sys")), check_vma=False)
```
